32 devices in a mesh: seq: 8 (over z, y), grp: 4 (over x, core).
Axes of the slice: x: 2, y: 2, z: 4, core: 2. Of those that a mesh axis runs over, the one named last changes fastest.
Arguments:
- hidden: bfloat16 [256, 8192], P('grp', 'seq'), may hold values from -6 to 6
- w_qkv: bfloat16 [8192, 10240], P('seq', 'grp'), may hold values from -0.0625 to 0.0625
- b_qkv: float32 [10240], P('grp'), may hold values from -3 to 3
- w_out: bfloat16 [8192, 8192], P('seq', 'grp'), may hold values from -0.0625 to 0.0625
- k_cache: bfloat16 [4, 32768, 1024], P('grp', 'seq'), may hold values from -600 to 600
- v_cache: bfloat16 [4, 32768, 1024], P('grp', 'seq'), may hold values from -6 to 6
- lengths: int32 [256], replicated, may hold values from 1 to 16384, as said below
- page_table: int32 [256, 128], replicated, may hold values from -1 to 255, as said below
- positions: int32 [3, 256], replicated, may hold values from 0 to 4095
- group_of: int32 [256], replicated, may hold values from 0 to 3, as said below
Outputs:
- mixed: bfloat16 [256, 8192], P('seq', 'grp')
The draws below stay inside these ranges and needn't reach their ends.
Inputs may be any that keep to these rules, and one draw needn't show every extreme that they name: `group_of`: each group serves exactly 64 requests. `lengths`: each group has a request of exactly 16384 cached positions. `page_table`: entry j of row r is the page of request r's group pool (page p lies on that group's device p // 32 of seq) that holds its positions j * 128 to (j + 1) * 128 - 1, for j < ceil(lengths[r] / 128); later entries are -1; no page belongs to two requests.
All inputs are finite; a program needn't handle non-finite values.
Results may differ from the reference program's by a relative error of at most 0.015.
The reference program's roundings to bfloat16 on the way count: a program that leaves them out, or rounds other values in their place, can miss the bound.
Values may be sent and summed in bfloat16 or wider, within the bound.
A program may use at most 128 MiB of HBM per device.

```python
import math
import jax
import jax.numpy as jnp
from jax import lax

D = 8192
HQ = 64
KVH = 8
HD = 128
REQ_GRP = 64
POOL = 32
PAGE = 128
QKV = 10240
MAXP = 128
REQ = 256
N_SEQ = 8
N_GRP = 4


def layout(key):
    base_key = jax.random.fold_in(key, 4242)
    key_group, key_weight, key_tail, key_place = jax.random.split(base_key, 4)
    group_pages = N_SEQ * POOL
    group_of = (jax.random.permutation(key_group, REQ).astype(jnp.int32) // REQ_GRP).astype(jnp.int32)
    served_order = jnp.argsort(group_of, stable=True).astype(jnp.int32)
    rank_of = jnp.zeros((REQ,), jnp.int32).at[served_order].set(jnp.arange(REQ, dtype=jnp.int32))
    leading = rank_of % REQ_GRP == 0
    exponent = jax.random.randint(key_weight, (REQ,), 0, 5).astype(jnp.int32)
    weight = jnp.left_shift(jnp.ones((REQ,), jnp.int32), exponent)
    member = group_of[:, None] == jnp.arange(N_GRP, dtype=jnp.int32)[None, :]
    group_weight = jnp.sum(jnp.where(member, weight[:, None], 0), axis=0).astype(jnp.int32)
    spare_pages = group_pages // 2 - REQ_GRP
    page_counts = 1 + spare_pages * weight // group_weight[group_of]
    page_counts = jnp.where(leading, MAXP, jnp.minimum(page_counts, MAXP)).astype(jnp.int32)
    tail_fill = jax.random.randint(key_tail, (REQ,), 1, PAGE + 1).astype(jnp.int32)
    lengths = (page_counts - 1) * PAGE + jnp.where(leading, PAGE, tail_fill)
    sorted_pages = page_counts[served_order].reshape(N_GRP, REQ_GRP)
    starts_sorted = (jnp.cumsum(sorted_pages, axis=1) - sorted_pages).reshape(REQ)
    starts = starts_sorted[rank_of]
    device_of = jnp.arange(group_pages, dtype=jnp.int32) // POOL
    priority = jax.random.randint(key_place, (N_GRP, group_pages), 0, 4096).astype(jnp.int32)
    priority = priority + device_of[None, :] * (6144 // N_SEQ)
    priority = priority * group_pages + jnp.arange(group_pages, dtype=jnp.int32)[None, :]
    placed = jnp.argsort(priority, axis=1).astype(jnp.int32)
    logical = jnp.arange(MAXP, dtype=jnp.int32)
    slot_index = jnp.minimum(starts[:, None] + logical[None, :], group_pages - 1)
    physical = placed[group_of[:, None], slot_index]
    page_table = jnp.where(logical[None, :] < page_counts[:, None], physical, -1)
    return (group_of.astype(jnp.int32), lengths.astype(jnp.int32), page_table.astype(jnp.int32))


def draw_group_of(key, part):
    return layout(key)[0]


def draw_lengths(key, part):
    return layout(key)[1]


def draw_page_table(key, part):
    return layout(key)[2]


def draw_k_cache(key, part):
    extent = (N_GRP, N_SEQ * POOL * PAGE, KVH * HD)
    drawn_keys = jnp.clip(jax.random.normal(jax.random.fold_in(key, 11), extent, jnp.float32), -6.0, 6.0)
    return drawn_keys.astype(jnp.bfloat16)


def touch_ends(drawn, stream_key, least, largest):
    place = [jax.random.randint(jax.random.fold_in(stream_key, axis), (), 0, length) for axis, length in enumerate(drawn.shape)]
    longest = drawn.shape.index(max(drawn.shape))
    next_to = place[:longest] + [(place[longest] + 1) % drawn.shape[longest]] + place[longest + 1:]
    return drawn.at[tuple(place)].set(least).at[tuple(next_to)].set(largest)


def shard_levels(stream_key, shape, cuts, low, high):
    def one(position, shards_of):
        draws = jax.random.uniform(jax.random.fold_in(jax.random.fold_in(stream_key, 6), position), (shards_of,), jnp.float32, low / len(cuts), high / len(cuts))
        return jnp.repeat(jnp.exp(draws), shape[position] // shards_of).reshape((-1,) + (1,) * (len(shape) - position - 1))

    factor_of = one(*cuts[0])
    for cut in cuts[1:]:
        factor_of = factor_of * one(*cut)
    return factor_of


def scatter_about(own_key, shape, width, most, shards=(), kind=jnp.bfloat16):
    result = jax.random.normal(own_key, shape, jnp.float32) * width
    if len(shards) > 0:
        result = shard_levels(own_key, shape, shards, -0.22, 0.18) * result
    return jnp.clip(result, min=-most, max=most).astype(kind)


def setup_inputs(seed: int = 0) -> dict:
    arg_keys = jax.random.split(jax.random.key(seed), 11)
    return {
        "hidden": scatter_about(arg_keys[0], (REQ, D), 1.0, 6.0, ((0, 4), (1, 8))),
        "w_qkv": scatter_about(arg_keys[1], (D, QKV), D ** -0.5, 0.0625, ((0, 8), (1, 4))),
        "b_qkv": scatter_about(arg_keys[2], (QKV,), 0.5, 3.0, ((0, 4),), jnp.float32),
        "w_out": scatter_about(arg_keys[3], (HQ * HD, D), (HQ * HD) ** -0.5, 0.0625, ((0, 8), (1, 4))),
        "k_cache": draw_k_cache(jax.random.fold_in(arg_keys[10], 71), 0),
        "v_cache": scatter_about(arg_keys[5], (N_GRP, N_SEQ * POOL * PAGE, KVH * HD), 1.0, 6.0, ((0, 4), (1, 8))),
        "lengths": draw_lengths(jax.random.fold_in(arg_keys[10], 71), 0),
        "page_table": draw_page_table(jax.random.fold_in(arg_keys[10], 71), 0),
        "positions": touch_ends(jax.random.randint(arg_keys[8], (3, REQ), 0, 4096), jax.random.fold_in(arg_keys[8], 1), 0, 4095).astype(jnp.int32),
        "group_of": draw_group_of(jax.random.fold_in(arg_keys[10], 71), 0),
    }


rope_base = 1000000.0
neg_fill = -1.0e30


def rotate_heads(values, places, col_start, head_dim, turned):
    row_count, col_count = values.shape
    columns = col_start + jnp.arange(col_count, dtype=jnp.int32)
    within = columns % head_dim
    freq_index = within % (head_dim // 2)
    inverse_freq = jnp.exp(freq_index.astype(jnp.float32) * (-2.0 * math.log(rope_base) / head_dim))
    section = jnp.where(freq_index < head_dim // 8, 0, jnp.where(freq_index < head_dim // 8 + 3 * head_dim // 16, 1, 2))
    place_float = places.astype(jnp.float32)
    chosen = jnp.where(section[None, :] == 0, place_float[0][:, None],
                       jnp.where(section[None, :] == 1, place_float[1][:, None], place_float[2][:, None]))
    angles = chosen * inverse_freq[None, :]
    halves = values.reshape(row_count, col_count // head_dim, 2, head_dim // 2)
    partner = jnp.concatenate([-halves[:, :, 1:], halves[:, :, :1]], axis=2).reshape(row_count, col_count)
    rotated = values * jnp.cos(angles) + partner * jnp.sin(angles)
    return jnp.where((columns < turned)[None, :], rotated, values)


def reference(hidden, w_qkv, b_qkv, w_out, k_cache, v_cache, lengths, page_table, positions, group_of):
    turned = (HQ + KVH) * HD
    group_q = HQ // KVH
    score_scale = HD ** -0.5
    projected = jnp.dot(hidden, w_qkv, preferred_element_type=jnp.float32) + b_qkv[None, :]
    fresh_rows = rotate_heads(projected, positions, 0, HD, turned).astype(jnp.bfloat16)
    query_rows = fresh_rows[:, : HQ * HD]
    key_new = fresh_rows[:, HQ * HD: turned]
    value_new = fresh_rows[:, turned:]
    group_pages = N_SEQ * POOL
    all_pages = N_GRP * group_pages
    page_counts = (lengths + PAGE - 1) // PAGE
    logical = jnp.arange(MAXP, dtype=jnp.int32)
    usable = logical[None, :] < page_counts[:, None]
    target = jnp.where(usable, group_of[:, None] * group_pages + page_table, all_pages).reshape(-1).astype(jnp.int32)
    page_owner = jnp.full((all_pages,), -1, jnp.int32).at[target].set(
        jnp.repeat(jnp.arange(REQ, dtype=jnp.int32), MAXP), mode="drop")
    page_number = jnp.zeros((all_pages,), jnp.int32).at[target].set(jnp.tile(logical, REQ), mode="drop")
    block_count = all_pages // POOL

    def one_block(block_items):
        key_block, value_block, owner_block, number_block = block_items
        present = owner_block >= 0
        holder = jnp.maximum(owner_block, 0)
        page_query = query_rows[holder].astype(jnp.float32).reshape(POOL, KVH, group_q, HD)
        scores = jnp.einsum("pkgd,ptkd->pkgt", page_query, key_block.astype(jnp.float32),
                            precision=lax.Precision.HIGHEST) * score_scale
        places_in = number_block[:, None] * PAGE + jnp.arange(PAGE, dtype=jnp.int32)[None, :]
        alive_rows = present[:, None] & (places_in < lengths[holder][:, None])
        alive_wide = alive_rows[:, None, None, :]
        page_max = jnp.max(jnp.where(alive_wide, scores, neg_fill), axis=3)
        weights = jnp.exp(jnp.where(alive_wide, scores - page_max[..., None], neg_fill))
        page_total = jnp.sum(weights, axis=3)
        rounded = weights.astype(jnp.bfloat16).astype(jnp.float32)
        page_out = jnp.einsum("pkgt,ptkd->pkgd", rounded, value_block.astype(jnp.float32),
                              precision=lax.Precision.HIGHEST)
        return page_max.reshape(POOL, HQ), page_total.reshape(POOL, HQ), page_out.reshape(POOL, HQ * HD)

    page_max, page_total, page_out = lax.map(one_block, (
        k_cache.reshape(block_count, POOL, PAGE, KVH, HD),
        v_cache.reshape(block_count, POOL, PAGE, KVH, HD),
        page_owner.reshape(block_count, POOL),
        page_number.reshape(block_count, POOL)))
    page_max = page_max.reshape(all_pages, HQ)
    page_total = page_total.reshape(all_pages, HQ)
    page_out = page_out.reshape(all_pages, HQ, HD)
    segment = jnp.where(page_owner >= 0, page_owner, REQ).astype(jnp.int32)
    new_score = jnp.einsum("rkgd,rkd->rkg", query_rows.astype(jnp.float32).reshape(REQ, KVH, group_q, HD),
                           key_new.astype(jnp.float32).reshape(REQ, KVH, HD),
                           precision=lax.Precision.HIGHEST).reshape(REQ, HQ) * score_scale
    page_peak = jnp.full((REQ + 1, HQ), neg_fill, jnp.float32).at[segment].max(page_max)
    peak_score = jnp.maximum(page_peak[:REQ], new_score)
    peak_wide = jnp.concatenate([peak_score, jnp.zeros((1, HQ), jnp.float32)], axis=0)
    factor = jnp.where((page_owner >= 0)[:, None], jnp.exp(page_max - peak_wide[segment]), 0.0)
    summed_total = jax.ops.segment_sum(page_total * factor, segment, REQ + 1)[:REQ]
    summed_out = jax.ops.segment_sum(page_out * factor[..., None], segment, REQ + 1)[:REQ]
    fresh_weight = jnp.exp(new_score - peak_score)
    value_heads = jnp.broadcast_to(value_new.astype(jnp.float32).reshape(REQ, KVH, 1, HD),
                                   (REQ, KVH, group_q, HD)).reshape(REQ, HQ, HD)
    numerator = summed_out + fresh_weight[..., None] * value_heads
    denominator = summed_total + fresh_weight
    attended = (numerator / denominator[..., None]).reshape(REQ, HQ * HD).astype(jnp.bfloat16)
    return jnp.dot(attended, w_out, preferred_element_type=jnp.float32).astype(jnp.bfloat16)
```

```python
import functools
import math

import jax
import jax.numpy as jnp
from jax import lax
from jax.experimental import pallas as pl
from jax.experimental.pallas import tpu as pltpu
from jax.sharding import PartitionSpec as P

HQ = 64
KVH = 8
HD = 128
PAGE = 128
LOW = 2
MESH = pl.DeviceIdType.MESH

rope_base = 1000000.0
neg_fill = -1e30


def greet(n_seq, n_grp):
    seq, grp = lax.axis_index("seq"), lax.axis_index("grp")
    barrier = pltpu.get_barrier_semaphore()
    for i in range(1, n_seq):
        pl.semaphore_signal(
            barrier, inc=1, device_id={"seq": lax.rem(seq + i, n_seq)}, device_id_type=MESH
        )
    for i in range(1, n_grp):
        pl.semaphore_signal(
            barrier, inc=1, device_id={"grp": lax.rem(grp + i, n_grp)}, device_id_type=MESH
        )
    pl.semaphore_wait(barrier, n_seq + n_grp - 2)


def send(src, dst, send_sem, recv_sem, axis, index):
    copy = pltpu.make_async_remote_copy(
        src_ref=src,
        dst_ref=dst,
        send_sem=send_sem,
        recv_sem=recv_sem,
        device_id={axis: index},
        device_id_type=MESH,
    )
    copy.start()
    return copy


def arrived(ref, sem):
    pltpu.make_async_copy(ref, ref, sem).wait()


def gather_groups(n_grp, own_ref, all_ref, send_sem, recv_sem):
    grp = lax.axis_index("grp")
    high_count = n_grp // LOW
    high, low = grp // LOW, lax.rem(grp, LOW)
    copies = [
        send(own_ref, all_ref.at[grp], send_sem.at[i - 1], recv_sem.at[grp], "grp",
             lax.rem(high + i, high_count) * LOW + low)
        for i in range(1, high_count)
    ]
    other = grp + 1 - 2 * low
    copies.append(
        send(own_ref, all_ref.at[grp], send_sem.at[high_count - 1], recv_sem.at[grp], "grp", other)
    )
    all_ref[grp] = own_ref[...]
    for i in range(1, high_count):
        block = lax.rem(high + high_count - i, high_count) * LOW + low
        arrived(all_ref.at[block], recv_sem.at[block])
        copies.append(
            send(all_ref.at[block], all_ref.at[block], send_sem.at[high_count - 1 + i],
                 recv_sem.at[block], "grp", other)
        )
    for h in range(high_count):
        block = h * LOW + 1 - low
        arrived(all_ref.at[block], recv_sem.at[block])
    return copies


def project_kernel(n_seq, n_grp, hidden_ref, perm_ref, w_hbm, bias_ref, cos_ref, sin_ref,
                   q_ref, nv_ref, hid_all, rows_ref, w_ref, own_ref, y_send, y_recv, z_send,
                   z_recv, turned_ref, d_send, d_recv, x_ref, wide_ref, block_ref, nv_send,
                   w_sem, g_send, g_recv, ys_sem, yr_sem, zs_sem, zr_sem, ds_sem, dr_sem,
                   qs_sem, qr_sem, ns_sem, nr_sem):
    pieces, depth, width = w_ref.shape
    seq, grp = lax.axis_index("seq"), lax.axis_index("grp")
    high_count = n_seq // LOW
    high, low = seq // LOW, lax.rem(seq, LOW)
    pair = seq + 1 - 2 * low
    half = rows_ref.shape[0] // LOW
    row_share = half // high_count
    share = row_share // n_grp
    piece_heads = width // HD
    block_heads = pieces * piece_heads
    head_share = HQ // n_seq
    group_q = HQ // KVH

    def fetch(p):
        return pltpu.make_async_copy(
            w_hbm.at[:, pl.ds(pl.multiple_of(p * width, width), width)], w_ref.at[p], w_sem.at[p]
        )

    for p in range(pieces):
        fetch(p).start()
    greet(n_seq, n_grp)
    hidden_sends = gather_groups(n_grp, hidden_ref, hid_all, g_send, g_recv)
    rows_ref[...] = jnp.dot(
        perm_ref[...], hid_all[...].reshape(-1, depth), preferred_element_type=jnp.float32
    ).astype(jnp.bfloat16)

    def y_copy(p):
        return pltpu.make_async_remote_copy(
            src_ref=y_send.at[p], dst_ref=y_recv.at[p], send_sem=ys_sem.at[p],
            recv_sem=yr_sem.at[p], device_id={"seq": pair}, device_id_type=MESH)

    def multiply(p, carry):
        fetch(p).wait()
        theirs = rows_ref[pl.ds(pl.multiple_of((1 - low) * half, half), half), :]
        y_send[p] = jnp.dot(theirs, w_ref[p], preferred_element_type=jnp.float32)
        y_copy(p).start()
        mine = rows_ref[pl.ds(pl.multiple_of(low * half, half), half), :]
        own_ref[p] = jnp.dot(mine, w_ref[p], preferred_element_type=jnp.float32)
        return carry

    lax.fori_loop(0, pieces, multiply, 0)

    def z_copy(p, i):
        peer = lax.rem(high + i, high_count)
        return pltpu.make_async_remote_copy(
            src_ref=z_send.at[p, peer], dst_ref=z_recv.at[p, i - 1], send_sem=zs_sem.at[p, i - 1],
            recv_sem=zr_sem.at[p, i - 1], device_id={"seq": peer * LOW + low},
            device_id_type=MESH)

    def spread(p):
        y_copy(p).wait_recv()
        z_send[p] = (own_ref[p] + y_recv[p]).reshape(high_count, row_share, width)
        for i in range(1, high_count):
            z_copy(p, i).start()

    def finish(p):
        total = z_send[p, high]
        for i in range(1, high_count):
            z_copy(p, i).wait_recv()
            total = total + z_recv[p, i - 1]
        total = total + bias_ref[p]
        for k in range(piece_heads):
            values = total[:, k * HD : (k + 1) * HD]
            rotated = values * cos_ref[...] + pltpu.roll(values, HD // 2, 1) * sin_ref[...]
            head = p * piece_heads + k
            values = jnp.where(grp * block_heads + head < HQ + KVH, rotated, values)
            for g in range(n_grp):
                turned_ref[g, pl.ds(head, share, stride=block_heads), :] = values[
                    g * share : (g + 1) * share
                ]

    spread(0)

    def step(p, carry):
        spread(p)
        finish(p - 1)
        return carry

    lax.fori_loop(1, pieces, step, 0)
    finish(pieces - 1)

    d_send[...] = turned_ref[...].astype(jnp.bfloat16)
    head_sends = []
    for i in range(1, n_grp):
        peer = lax.rem(grp + i, n_grp)
        head_sends.append(
            send(d_send.at[peer], d_recv.at[i - 1], ds_sem.at[i - 1], dr_sem.at[i - 1], "grp", peer)
        )
    x_ref[grp] = d_send[grp].astype(jnp.float32)
    for i in range(1, n_grp):
        head_sends[i - 1].wait_recv()
        x_ref[lax.rem(grp + n_grp - i, n_grp)] = d_recv[i - 1].astype(jnp.float32)

    def head_rows(head):
        return x_ref[head // block_heads, pl.ds(head % block_heads, share, stride=block_heads), :]

    for head in range(HQ):
        wide_ref[pl.ds(head, share, stride=HQ), :] = head_rows(head)
    block_ref[...] = wide_ref[...].reshape(share, HQ, HD).astype(jnp.bfloat16)

    def rows_of(index):
        return q_ref.at[pl.ds(index * share, share)]

    q_sends = []
    for i in range(1, high_count):
        peer = lax.rem(high + i, high_count) * LOW + low
        q_sends.append(
            send(block_ref, rows_of(seq), qs_sem.at[i - 1], qr_sem.at[seq], "seq", peer)
        )
    q_sends.append(
        send(block_ref, rows_of(seq), qs_sem.at[high_count - 1], qr_sem.at[seq], "seq", pair)
    )
    q_ref[pl.ds(seq * share, share)] = block_ref[...]

    lane = lax.broadcasted_iota(jnp.int32, (share, HD), 1)
    for peer in range(n_seq):
        kv = peer * head_share // group_q
        scores = jnp.zeros((share, HD), jnp.float32)
        for k in range(head_share):
            head = peer * head_share + k
            key = head_rows(HQ + head // group_q)
            score = jnp.sum(head_rows(head) * key, axis=1, keepdims=True) * (HD**-0.5)
            scores = jnp.where(lane == k, score, scores)
        nv_send[peer, 0] = scores
        nv_send[peer, 1] = head_rows(HQ + KVH + kv)
    nv_sends = []
    for i in range(1, n_seq):
        peer = lax.rem(seq + i, n_seq)
        nv_sends.append(
            send(nv_send.at[peer], nv_ref.at[seq], ns_sem.at[i - 1], nr_sem.at[seq], "seq", peer)
        )
    nv_ref[seq] = nv_send[seq]

    for i in range(1, high_count):
        block = lax.rem(high + high_count - i, high_count) * LOW + low
        arrived(rows_of(block), qr_sem.at[block])
        q_sends.append(
            send(rows_of(block), rows_of(block), qs_sem.at[high_count - 1 + i], qr_sem.at[block],
                 "seq", pair)
        )
    for h in range(high_count):
        block = h * LOW + 1 - low
        arrived(rows_of(block), qr_sem.at[block])
    for i in range(1, n_seq):
        block = lax.rem(seq + i, n_seq)
        arrived(nv_ref.at[block], nr_sem.at[block])

    def drain(p, carry):
        y_copy(p).wait_send()
        for i in range(1, high_count):
            z_copy(p, i).wait_send()
        return carry

    lax.fori_loop(0, pieces, drain, 0)
    for copy in hidden_sends + head_sends + q_sends + nv_sends:
        copy.wait_send()


def project(n_seq, n_grp, hidden, perm, w_qkv, bias, cosine, sine):
    group_size, depth = hidden.shape
    request_total = perm.shape[0]
    col_count = w_qkv.shape[1]
    pieces = math.gcd(col_count // HD, 5)
    width = col_count // pieces
    half = request_total // LOW
    high_count = n_seq // LOW
    row_share = half // high_count
    share = row_share // n_grp
    block_rows = share * col_count // HD
    dma = pltpu.SemaphoreType.DMA
    vmem = pl.BlockSpec(memory_space=pltpu.VMEM)
    return pl.pallas_call(
        functools.partial(project_kernel, n_seq, n_grp),
        out_shape=[
            jax.ShapeDtypeStruct((group_size, HQ, HD), jnp.bfloat16),
            jax.ShapeDtypeStruct((n_seq, 2, share, HD), jnp.float32),
        ],
        in_specs=[vmem, vmem, pl.BlockSpec(memory_space=pl.ANY), vmem, vmem, vmem],
        out_specs=[vmem, vmem],
        scratch_shapes=[
            pltpu.VMEM((n_grp, group_size, depth), jnp.bfloat16),
            pltpu.VMEM((request_total, depth), jnp.bfloat16),
            pltpu.VMEM((pieces, depth, width), jnp.bfloat16),
            pltpu.VMEM((pieces, half, width), jnp.float32),
            pltpu.VMEM((pieces, half, width), jnp.float32),
            pltpu.VMEM((pieces, half, width), jnp.float32),
            pltpu.VMEM((pieces, high_count, row_share, width), jnp.float32),
            pltpu.VMEM((pieces, high_count - 1, row_share, width), jnp.float32),
            pltpu.VMEM((n_grp, block_rows, HD), jnp.float32),
            pltpu.VMEM((n_grp, block_rows, HD), jnp.bfloat16),
            pltpu.VMEM((n_grp - 1, block_rows, HD), jnp.bfloat16),
            pltpu.VMEM((n_grp, block_rows, HD), jnp.float32),
            pltpu.VMEM((share * HQ, HD), jnp.float32),
            pltpu.VMEM((share, HQ, HD), jnp.bfloat16),
            pltpu.VMEM((n_seq, 2, share, HD), jnp.float32),
            dma((pieces,)),
            dma((2 * n_grp,)),
            dma((n_grp,)),
            dma((pieces,)),
            dma((pieces,)),
            dma((pieces, high_count - 1)),
            dma((pieces, high_count - 1)),
            dma((n_grp - 1,)),
            dma((n_grp - 1,)),
            dma((2 * high_count,)),
            dma((n_seq,)),
            dma((n_seq - 1,)),
            dma((n_seq,)),
        ],
        compiler_params=pltpu.CompilerParams(
            collective_id=0, has_side_effects=True, vmem_limit_bytes=56 * 1024 * 1024
        ),
        cost_estimate=pl.CostEstimate(
            flops=2 * request_total * depth * col_count,
            bytes_accessed=2 * depth * col_count,
            transcendentals=0,
        ),
    )(hidden, perm, w_qkv, bias.reshape(pieces, 1, width), cosine, sine)


def attend_pages(block_pages, owner_ref, live_ref, rows_ref, key_ref, value_ref, out_ref, stat_ref,
                 wide_ref):
    step = pl.program_id(0)
    group_q = HQ // KVH
    width = KVH * HD
    pool_pages = out_ref.shape[1]

    @pl.when(step == 0)
    def _():
        stat_ref[...] = jnp.zeros_like(stat_ref)

    row_head = lax.broadcasted_iota(jnp.int32, (HQ, width), 0) // group_q
    col_head = lax.broadcasted_iota(jnp.int32, (HQ, width), 1) // HD
    own_head = (row_head == col_head).astype(jnp.float32).astype(jnp.bfloat16)
    place = lax.broadcasted_iota(jnp.int32, (HQ, PAGE), 1)
    lane = lax.broadcasted_iota(jnp.int32, (HQ, HD), 1)
    stat = stat_ref[...].reshape(HQ, HD)
    for j in range(block_pages):
        page = step * block_pages + j
        owner = owner_ref[page]
        alive = place < live_ref[page]
        query = rows_ref[owner]
        spread = jnp.concatenate([query] * KVH, axis=1) * own_head
        keys = key_ref[0, j * PAGE : (j + 1) * PAGE, :]
        values = value_ref[0, j * PAGE : (j + 1) * PAGE, :]
        scores = lax.dot_general(
            spread, keys, (((1,), (1,)), ((), ())), preferred_element_type=jnp.float32
        ) * (HD**-0.5)
        scores = jnp.where(alive, scores, neg_fill)
        page_max = jnp.max(scores, axis=1, keepdims=True)
        weights = jnp.where(alive, jnp.exp(scores - page_max), 0.0)
        page_total = jnp.sum(weights, axis=1, keepdims=True)
        wide = jnp.dot(weights.astype(jnp.bfloat16), values, preferred_element_type=jnp.float32)
        page_out = jnp.concatenate(
            [
                wide[h * group_q : (h + 1) * group_q, h * HD : (h + 1) * HD]
                for h in range(KVH)
            ],
            axis=0,
        )
        wide_ref[pl.ds(page, HQ, stride=pool_pages), :] = page_out
        holder = jnp.where(live_ref[page] > 0, owner, -1).astype(jnp.float32)
        stat = jnp.where(lane == page, page_max, stat)
        stat = jnp.where(lane == pool_pages + page, page_total, stat)
        stat = jnp.where(lane == 2 * pool_pages + page, holder, stat)
    stat_ref[...] = stat.reshape(stat_ref.shape)

    @pl.when(step == pl.num_programs(0) - 1)
    def _():
        out_ref[...] = wide_ref[...].reshape(out_ref.shape).astype(jnp.bfloat16)


def local_attention(n_seq, owner, live, rows, k_cache, v_cache):
    group_size = rows.shape[0]
    pool_pages = k_cache.shape[1] // PAGE
    block_pages = math.gcd(pool_pages, 4)
    cache_spec = pl.BlockSpec((1, block_pages * PAGE, KVH * HD), lambda i, *_: (0, i, 0))
    out_shape = [
        jax.ShapeDtypeStruct((HQ, pool_pages, HD), jnp.bfloat16),
        jax.ShapeDtypeStruct((n_seq, HQ // n_seq, HD), jnp.float32),
    ]
    return pl.pallas_call(
        functools.partial(attend_pages, block_pages),
        grid_spec=pltpu.PrefetchScalarGridSpec(
            num_scalar_prefetch=2,
            grid=(pool_pages // block_pages,),
            in_specs=[
                pl.BlockSpec(rows.shape, lambda i, *_: (0, 0, 0)),
                cache_spec,
                cache_spec,
            ],
            out_specs=[
                pl.BlockSpec(shape.shape, lambda i, *_: (0, 0, 0)) for shape in out_shape
            ],
            scratch_shapes=[pltpu.VMEM((HQ * pool_pages, HD), jnp.float32)],
        ),
        out_shape=out_shape,
        compiler_params=pltpu.CompilerParams(
            dimension_semantics=("arbitrary",), vmem_limit_bytes=56 * 1024 * 1024
        ),
        cost_estimate=pl.CostEstimate(
            flops=4 * pool_pages * HQ * PAGE * KVH * HD,
            bytes_accessed=4 * pool_pages * PAGE * KVH * HD,
            transcendentals=pool_pages * HQ * PAGE,
        ),
    )(owner, live, rows, k_cache, v_cache)


def mix_kernel(n_seq, n_grp, out_ref, stat_ref, nv_ref, perm_ref, w_hbm, mixed_ref,
               o_all, s_all, att_ref, att_all, rows_ref, w_ref, own_ref, y_send, y_recv, z_keep,
               z_send, z_recv, w_sem, os_sem, or_sem, ss_sem, sr_sem, g_send, g_recv,
               ys_sem, yr_sem, zs_sem, zr_sem):
    pieces, depth, width = w_ref.shape
    seq = lax.axis_index("seq")
    high_count = n_seq // LOW
    high, low = seq // LOW, lax.rem(seq, LOW)
    pair = seq + 1 - 2 * low
    half = rows_ref.shape[0] // LOW
    row_share = half // high_count
    head_share = HQ // n_seq
    pool_pages = out_ref.shape[1]
    slots = n_seq * pool_pages
    packed = HD // pool_pages
    group_size = att_ref.shape[0]

    def fetch(p):
        return pltpu.make_async_copy(
            w_hbm.at[:, pl.ds(pl.multiple_of(p * width, width), width)], w_ref.at[p], w_sem.at[p]
        )

    for p in range(pieces):
        fetch(p).start()
    greet(n_seq, n_grp)
    slot_sends = []
    for i in range(1, n_seq):
        peer = lax.rem(seq + i, n_seq)
        slot_sends.append(
            send(stat_ref.at[peer], s_all.at[seq], ss_sem.at[i - 1], sr_sem.at[seq], "seq", peer)
        )
        slot_sends.append(
            send(out_ref.at[pl.ds(peer * head_share, head_share)], o_all.at[seq], os_sem.at[i - 1],
                 or_sem.at[seq], "seq", peer)
        )
    s_all[seq] = stat_ref[seq]
    o_all[seq] = out_ref[pl.ds(seq * head_share, head_share)]
    for i in range(1, n_seq):
        peer = lax.rem(seq + i, n_seq)
        arrived(s_all.at[peer], sr_sem.at[peer])

    spot = lax.broadcasted_iota(jnp.int32, (head_share, HD), 1) // pool_pages

    def lined_up(field):
        tiles = []
        for first in range(0, n_seq, packed):
            tile = jnp.zeros((head_share, HD), jnp.float32)
            for k in range(packed):
                shift = (HD + (k - field) * pool_pages) % HD
                source = s_all[first + k]
                tile = jnp.where(spot == k, pltpu.roll(source, shift, 1) if shift else source, tile)
            tiles.append(tile)
        return jnp.concatenate(tiles, axis=1)

    tops, totals, holders = lined_up(0), lined_up(1), lined_up(2)
    request = lax.broadcasted_iota(jnp.int32, (group_size, slots), 0).astype(jnp.float32)
    held = request == holders[:1, :]
    fresh_scores = nv_ref[:, 0].reshape(group_size, HD)
    fresh_values = nv_ref[:, 1].reshape(group_size, HD)
    for i in range(1, n_seq):
        peer = lax.rem(seq + i, n_seq)
        arrived(o_all.at[peer], or_sem.at[peer])
    for k in range(head_share):
        top = jnp.where(held, tops[k : k + 1, :], neg_fill)
        fresh = fresh_scores[:, k : k + 1]
        peak = jnp.maximum(jnp.max(top, axis=1, keepdims=True), fresh)
        factor = jnp.where(held, jnp.exp(top - peak), 0.0)
        fresh_weight = jnp.exp(fresh - peak)
        denominator = jnp.sum(factor * totals[k : k + 1, :], axis=1, keepdims=True) + fresh_weight
        coarse = factor.astype(jnp.bfloat16)
        fine = (factor - coarse.astype(jnp.float32)).astype(jnp.bfloat16)
        outs = o_all[:, k].reshape(slots, HD)
        numerator = (
            jnp.dot(coarse, outs, preferred_element_type=jnp.float32)
            + jnp.dot(fine, outs, preferred_element_type=jnp.float32)
            + fresh_weight * fresh_values
        )
        att_ref[:, k * HD : (k + 1) * HD] = (numerator / denominator).astype(jnp.bfloat16)

    att_sends = gather_groups(n_grp, att_ref, att_all, g_send, g_recv)
    rows_ref[...] = jnp.dot(
        perm_ref[...], att_all[...].reshape(-1, depth), preferred_element_type=jnp.float32
    ).astype(jnp.bfloat16)

    def y_copy(p):
        return pltpu.make_async_remote_copy(
            src_ref=y_send.at[p], dst_ref=y_recv.at[p], send_sem=ys_sem.at[p],
            recv_sem=yr_sem.at[p], device_id={"seq": pair}, device_id_type=MESH)

    def multiply(p, carry):
        fetch(p).wait()
        theirs = rows_ref[pl.ds(pl.multiple_of((1 - low) * half, half), half), :]
        y_send[p] = jnp.dot(theirs, w_ref[p], preferred_element_type=jnp.float32).astype(
            jnp.bfloat16
        )
        y_copy(p).start()
        mine = rows_ref[pl.ds(pl.multiple_of(low * half, half), half), :]
        own_ref[p] = jnp.dot(mine, w_ref[p], preferred_element_type=jnp.float32)
        return carry

    lax.fori_loop(0, pieces, multiply, 0)

    def z_copy(p, i):
        peer = lax.rem(high + i, high_count)
        return pltpu.make_async_remote_copy(
            src_ref=z_send.at[p, peer], dst_ref=z_recv.at[p, i - 1], send_sem=zs_sem.at[p, i - 1],
            recv_sem=zr_sem.at[p, i - 1], device_id={"seq": peer * LOW + low},
            device_id_type=MESH)

    def spread(p, carry):
        y_copy(p).wait_recv()
        z_keep[p] = (own_ref[p] + y_recv[p].astype(jnp.float32)).reshape(
            high_count, row_share, width
        )
        z_send[p] = z_keep[p].astype(jnp.bfloat16)
        for i in range(1, high_count):
            z_copy(p, i).start()
        return carry

    lax.fori_loop(0, pieces, spread, 0)
    for p in range(pieces):
        total = z_keep[p, high]
        for i in range(1, high_count):
            z_copy(p, i).wait_recv()
            total = total + z_recv[p, i - 1].astype(jnp.float32)
        mixed_ref[:, p * width : (p + 1) * width] = total.astype(jnp.bfloat16)

    def drain(p, carry):
        y_copy(p).wait_send()
        for i in range(1, high_count):
            z_copy(p, i).wait_send()
        return carry

    lax.fori_loop(0, pieces, drain, 0)
    for copy in slot_sends + att_sends:
        copy.wait_send()


def mix(n_seq, n_grp, outs, stats, nv, perm, w_out):
    request_total = perm.shape[0]
    group_size = request_total // n_grp
    depth, col_count = w_out.shape
    pieces = math.gcd(col_count // HD, 4)
    width = col_count // pieces
    half = request_total // LOW
    high_count = n_seq // LOW
    row_share = half // high_count
    head_share = HQ // n_seq
    pool_pages = outs.shape[1]
    dma = pltpu.SemaphoreType.DMA
    vmem = pl.BlockSpec(memory_space=pltpu.VMEM)
    return pl.pallas_call(
        functools.partial(mix_kernel, n_seq, n_grp),
        out_shape=jax.ShapeDtypeStruct((row_share, col_count), jnp.bfloat16),
        in_specs=[vmem, vmem, vmem, vmem, pl.BlockSpec(memory_space=pl.ANY)],
        out_specs=vmem,
        scratch_shapes=[
            pltpu.VMEM((n_seq, head_share, pool_pages, HD), jnp.bfloat16),
            pltpu.VMEM((n_seq, head_share, HD), jnp.float32),
            pltpu.VMEM((group_size, depth), jnp.bfloat16),
            pltpu.VMEM((n_grp, group_size, depth), jnp.bfloat16),
            pltpu.VMEM((request_total, depth), jnp.bfloat16),
            pltpu.VMEM((pieces, depth, width), jnp.bfloat16),
            pltpu.VMEM((pieces, half, width), jnp.float32),
            pltpu.VMEM((pieces, half, width), jnp.bfloat16),
            pltpu.VMEM((pieces, half, width), jnp.bfloat16),
            pltpu.VMEM((pieces, high_count, row_share, width), jnp.float32),
            pltpu.VMEM((pieces, high_count, row_share, width), jnp.bfloat16),
            pltpu.VMEM((pieces, high_count - 1, row_share, width), jnp.bfloat16),
            dma((pieces,)),
            dma((n_seq - 1,)),
            dma((n_seq,)),
            dma((n_seq - 1,)),
            dma((n_seq,)),
            dma((2 * n_grp,)),
            dma((n_grp,)),
            dma((pieces,)),
            dma((pieces,)),
            dma((pieces, high_count - 1)),
            dma((pieces, high_count - 1)),
        ],
        compiler_params=pltpu.CompilerParams(
            collective_id=1, has_side_effects=True, vmem_limit_bytes=56 * 1024 * 1024
        ),
        cost_estimate=pl.CostEstimate(
            flops=2 * request_total * depth * col_count,
            bytes_accessed=2 * depth * col_count,
            transcendentals=0,
        ),
    )(outs, stats, nv, perm, w_out)


def rope_tables(places):
    freq_index = jnp.arange(HD // 2, dtype=jnp.int32)
    inverse_freq = jnp.exp(freq_index.astype(jnp.float32) * (-2.0 * math.log(rope_base) / HD))
    section = jnp.where(
        freq_index < HD // 8, 0, jnp.where(freq_index < HD // 8 + 3 * HD // 16, 1, 2)
    )
    place_float = places.astype(jnp.float32)
    chosen = jnp.where(
        section[None, :] == 0,
        place_float[0][:, None],
        jnp.where(section[None, :] == 1, place_float[1][:, None], place_float[2][:, None]),
    )
    angles = chosen * inverse_freq[None, :]
    cosine, sine = jnp.cos(angles), jnp.sin(angles)
    return jnp.concatenate([cosine, cosine], 1), jnp.concatenate([-sine, sine], 1)


def shards(hidden, w_qkv, b_qkv, w_out, k_cache, v_cache, lengths, page_table, positions, group_of):
    n_seq = lax.axis_size("seq")
    n_grp = lax.axis_size("grp")
    seq_index = lax.axis_index("seq")
    grp_index = lax.axis_index("grp")
    request_total = group_of.shape[0]
    group_size = request_total // n_grp
    share = group_size // n_seq
    high_count = n_seq // LOW
    row_share = request_total // n_seq
    request_ids = jnp.arange(request_total, dtype=jnp.int32)
    before = (group_of[None, :] < group_of[:, None]) | (group_of[None, :] == group_of[:, None]) & (
        request_ids[None, :] < request_ids[:, None]
    )
    served_at = jnp.sum(before.astype(jnp.int32), axis=1)
    rank = served_at % group_size
    holder = rank // share
    sent_at = (
        ((holder % LOW) * high_count + holder // LOW) * n_grp + served_at // group_size
    ) * share + rank % share
    in_perm = sent_at[None, :] == request_ids[:, None]
    my_start = ((seq_index % LOW) * high_count + seq_index // LOW) * row_share
    my_rows = (
        my_start + jnp.arange(row_share, dtype=jnp.int32)[:, None] == sent_at[None, :]
    )
    places = jnp.sum(jnp.where(my_rows[None], positions[:, None, :], 0), axis=2)
    cosine, sine = rope_tables(places)
    rows, nv = project(
        n_seq, n_grp, hidden, in_perm.astype(jnp.bfloat16), w_qkv, b_qkv, cosine, sine
    )

    placed_at = served_at[None, :] == request_ids[:, None]
    served_order = jnp.sum(jnp.where(placed_at, request_ids[None, :], 0), axis=1)
    served_ids = lax.dynamic_slice_in_dim(served_order, grp_index * group_size, group_size, 0)
    served_len = lengths[served_ids]
    served_table = page_table[served_ids]
    most_pages = page_table.shape[1]
    page_counts = (served_len + PAGE - 1) // PAGE
    logical = jnp.arange(most_pages, dtype=jnp.int32)
    pool_pages = k_cache.shape[1] // PAGE
    local_page = served_table - seq_index * pool_pages
    usable = (
        (logical[None, :] < page_counts[:, None]) & (local_page >= 0) & (local_page < pool_pages)
    )
    pool_ids = jnp.arange(pool_pages, dtype=jnp.int32)
    matched = usable[:, :, None] & (local_page[:, :, None] == pool_ids[None, None, :])
    owner_ids = jnp.arange(group_size, dtype=jnp.int32)
    left = served_len[:, None] - logical[None, :] * PAGE
    live = jnp.max(jnp.where(matched, left[:, :, None], 0), axis=(0, 1))
    owner = jnp.max(jnp.where(matched, owner_ids[:, None, None], 0), axis=(0, 1))
    outs, stats = local_attention(n_seq, owner, live, rows, k_cache, v_cache)

    back_at = served_at.reshape(high_count, LOW, row_share).transpose(1, 0, 2).reshape(-1)
    out_perm = back_at[:, None] == request_ids[None, :]
    return mix(n_seq, n_grp, outs, stats, nv, out_perm.astype(jnp.bfloat16), w_out)


def solution(mesh):
    placed = (
        P("grp", "seq"),
        P("seq", "grp"),
        P("grp"),
        P("seq", "grp"),
        P("grp", "seq", None),
        P("grp", "seq", None),
        P(),
        P(),
        P(),
        P(),
    )
    return jax.shard_map(
        shards, mesh=mesh, in_specs=placed, out_specs=P("seq", "grp"), check_vma=False
    )
```

```python
import functools
import math

import jax
import jax.numpy as jnp
from jax import lax
from jax.experimental import pallas as pl
from jax.experimental.pallas import tpu as pltpu
from jax.sharding import PartitionSpec as P

HQ = 64
KVH = 8
HD = 128
PAGE = 128
LOW = 2
MESH = pl.DeviceIdType.MESH

rope_base = 1000000.0
neg_fill = -1e30


def greet(n_seq, n_grp):
    seq, grp = lax.axis_index("seq"), lax.axis_index("grp")
    barrier = pltpu.get_barrier_semaphore()
    for i in range(1, n_seq):
        pl.semaphore_signal(
            barrier, inc=1, device_id={"seq": lax.rem(seq + i, n_seq)}, device_id_type=MESH
        )
    for i in range(1, n_grp):
        pl.semaphore_signal(
            barrier, inc=1, device_id={"grp": lax.rem(grp + i, n_grp)}, device_id_type=MESH
        )
    pl.semaphore_wait(barrier, n_seq + n_grp - 2)


def send(src, dst, send_sem, recv_sem, axis, index):
    copy = pltpu.make_async_remote_copy(
        src_ref=src,
        dst_ref=dst,
        send_sem=send_sem,
        recv_sem=recv_sem,
        device_id={axis: index},
        device_id_type=MESH,
    )
    copy.start()
    return copy


def arrived(ref, sem):
    pltpu.make_async_copy(ref, ref, sem).wait()


def gather_start(n_grp, own_ref, all_ref, send_sem, recv_sem):
    grp = lax.axis_index("grp")
    high_count = n_grp // LOW
    high, low = grp // LOW, lax.rem(grp, LOW)
    copies = [
        send(own_ref, all_ref.at[grp], send_sem.at[i - 1], recv_sem.at[grp], "grp",
             lax.rem(high + i, high_count) * LOW + low)
        for i in range(1, high_count)
    ]
    copies.append(
        send(own_ref, all_ref.at[grp], send_sem.at[high_count - 1], recv_sem.at[grp], "grp",
             grp + 1 - 2 * low)
    )
    all_ref[grp] = own_ref[...]
    return copies


def gather_relay(n_grp, all_ref, send_sem, recv_sem):
    grp = lax.axis_index("grp")
    high_count = n_grp // LOW
    high, low = grp // LOW, lax.rem(grp, LOW)
    copies = []
    for i in range(1, high_count):
        block = lax.rem(high + high_count - i, high_count) * LOW + low
        arrived(all_ref.at[block], recv_sem.at[block])
        copies.append(
            send(all_ref.at[block], all_ref.at[block], send_sem.at[high_count - 1 + i],
                 recv_sem.at[block], "grp", grp + 1 - 2 * low)
        )
    return copies


def gather_finish(n_grp, all_ref, recv_sem):
    low = lax.rem(lax.axis_index("grp"), LOW)
    for h in range(n_grp // LOW):
        block = h * LOW + 1 - low
        arrived(all_ref.at[block], recv_sem.at[block])


def reduce_scatter(n_seq, rows_ref, w_ref, fetch, own_ref, y_send, y_recv, z_send, z_recv, sems,
                   finish):
    ys_sem, yr_sem, zs_sem, zr_sem = sems
    pieces, _, width = w_ref.shape
    seq = lax.axis_index("seq")
    high_count = n_seq // LOW
    high, low = seq // LOW, lax.rem(seq, LOW)
    half = rows_ref.shape[0] // LOW
    row_share = half // high_count
    wire = y_send.dtype

    def y_copy(p):
        return pltpu.make_async_remote_copy(
            src_ref=y_send.at[p], dst_ref=y_recv.at[p], send_sem=ys_sem.at[p],
            recv_sem=yr_sem.at[p], device_id={"seq": seq + 1 - 2 * low}, device_id_type=MESH)

    def z_copy(p, i):
        peer = lax.rem(high + i, high_count)
        return pltpu.make_async_remote_copy(
            src_ref=z_send.at[p, peer], dst_ref=z_recv.at[p, i - 1], send_sem=zs_sem.at[p, i - 1],
            recv_sem=zr_sem.at[p, i - 1], device_id={"seq": peer * LOW + low},
            device_id_type=MESH)

    def multiply(p, carry):
        fetch(p).wait()
        theirs = rows_ref[pl.ds(pl.multiple_of((1 - low) * half, half), half), :]
        y_send[p] = jnp.dot(theirs, w_ref[p], preferred_element_type=jnp.float32).astype(wire)
        y_copy(p).start()
        mine = rows_ref[pl.ds(pl.multiple_of(low * half, half), half), :]
        own_ref[p] = jnp.dot(mine, w_ref[p], preferred_element_type=jnp.float32).reshape(
            high_count, row_share, width
        )
        return carry

    def spread(p):
        y_copy(p).wait_recv()
        summed = own_ref[p] + y_recv[p].astype(jnp.float32).reshape(high_count, row_share, width)
        own_ref[p] = summed
        z_send[p] = summed.astype(wire)
        for i in range(1, high_count):
            z_copy(p, i).start()

    def collect(p):
        total = own_ref[p, high]
        for i in range(1, high_count):
            z_copy(p, i).wait_recv()
            total = total + z_recv[p, i - 1].astype(jnp.float32)
        finish(p, total)

    def step(p, carry):
        spread(p)
        collect(p - 1)
        return carry

    def drain(p, carry):
        y_copy(p).wait_send()
        for i in range(1, high_count):
            z_copy(p, i).wait_send()
        return carry

    lax.fori_loop(0, pieces, multiply, 0)
    spread(0)
    lax.fori_loop(1, pieces, step, 0)
    collect(pieces - 1)
    return lambda: lax.fori_loop(0, pieces, drain, 0)


def step_kernel(n_seq, n_grp, owner_ref, live_ref, hidden_ref, perm_ref, back_ref, bias_ref,
                cos_ref, sin_ref, w_in_hbm, w_out_hbm, k_hbm, v_hbm, mixed_ref,
                key_ref, value_ref, w_in_ref, w_out_ref, hid_all, rows_ref, p_own, p_ys, p_yr,
                p_zs, p_zr, turned_ref, d_send, d_recv, x_ref, wide_ref, block_ref, q_ref, nv_send,
                nv_ref, page_ref, stat_ref, o_send, o_all, s_all, att_ref, att_all, m_own, m_ys,
                m_yr, m_zs, m_zr, w_in_sem, w_out_sem, kv_sem, hs_sem, hr_sem, p_ys_sem, p_yr_sem,
                p_zs_sem, p_zr_sem, ds_sem, dr_sem, qs_sem, qf_sem, qr_sem, ns_sem, nr_sem, os_sem,
                or_sem, ss_sem, sr_sem, as_sem, ar_sem, m_ys_sem, m_yr_sem, m_zs_sem, m_zr_sem):
    seq, grp = lax.axis_index("seq"), lax.axis_index("grp")
    high_count = n_seq // LOW
    high, low = seq // LOW, lax.rem(seq, LOW)
    pair = seq + 1 - 2 * low
    in_pieces, depth, in_width = w_in_ref.shape
    out_pieces, out_depth, out_width = w_out_ref.shape
    parts = hid_all.shape[0]
    share = block_ref.shape[0]
    piece_heads = in_width // HD
    block_heads = in_pieces * piece_heads
    head_share = HQ // n_seq
    group_q = HQ // KVH
    group_size = share * n_seq

    def in_fetch(p):
        return pltpu.make_async_copy(
            w_in_hbm.at[:, pl.ds(pl.multiple_of(p * in_width, in_width), in_width)],
            w_in_ref.at[p], w_in_sem.at[p])

    def out_fetch(p):
        return pltpu.make_async_copy(
            w_out_hbm.at[:, pl.ds(pl.multiple_of(p * out_width, out_width), out_width)],
            w_out_ref.at[p], w_out_sem.at[p])

    key_copy = pltpu.make_async_copy(k_hbm.at[0], key_ref, kv_sem.at[0])
    value_copy = pltpu.make_async_copy(v_hbm.at[0], value_ref, kv_sem.at[1])
    for p in range(in_pieces):
        in_fetch(p).start()
    greet(n_seq, n_grp)

    sends = []
    part = depth // parts
    for a in range(parts):
        sends += gather_start(n_grp, hidden_ref.at[:, a * part : (a + 1) * part], hid_all.at[a],
                              hs_sem.at[a], hr_sem.at[a])
    key_copy.start()
    value_copy.start()
    for p in range(out_pieces):
        out_fetch(p).start()
    for a in range(parts):
        sends += gather_relay(n_grp, hid_all.at[a], hs_sem.at[a], hr_sem.at[a])
    for a in range(parts):
        gather_finish(n_grp, hid_all.at[a], hr_sem.at[a])
        rows_ref[:, a * part : (a + 1) * part] = jnp.dot(
            perm_ref[...], hid_all[a].reshape(-1, part), preferred_element_type=jnp.float32
        ).astype(jnp.bfloat16)

    def turn(p, total):
        for k in range(piece_heads):
            head = p * piece_heads + k
            values = total[:, k * HD : (k + 1) * HD] + bias_ref[pl.ds(head, 1), :]
            rotated = values * cos_ref[...] + pltpu.roll(values, HD // 2, 1) * sin_ref[...]
            values = jnp.where(grp * block_heads + head < HQ + KVH, rotated, values)
            for g in range(n_grp):
                turned_ref[g, pl.ds(head, share, stride=block_heads), :] = values[
                    g * share : (g + 1) * share
                ]

    drain_in = reduce_scatter(n_seq, rows_ref, w_in_ref, in_fetch, p_own, p_ys, p_yr, p_zs, p_zr,
                              (p_ys_sem, p_yr_sem, p_zs_sem, p_zr_sem), turn)

    d_send[...] = turned_ref[...].astype(jnp.bfloat16)
    head_sends = []
    for i in range(1, n_grp):
        peer = lax.rem(grp + i, n_grp)
        head_sends.append(
            send(d_send.at[peer], d_recv.at[i - 1], ds_sem.at[i - 1], dr_sem.at[i - 1], "grp", peer)
        )
    x_ref[grp] = d_send[grp].astype(jnp.float32)
    for i in range(1, n_grp):
        head_sends[i - 1].wait_recv()
        x_ref[lax.rem(grp + n_grp - i, n_grp)] = d_recv[i - 1].astype(jnp.float32)
    sends += head_sends

    def head_rows(head):
        return x_ref[head // block_heads, pl.ds(head % block_heads, share, stride=block_heads), :]

    for head in range(HQ):
        wide_ref[pl.ds(head, share, stride=HQ), :] = head_rows(head)
    block_ref[...] = wide_ref[...].reshape(share, HQ, HD).astype(jnp.bfloat16)

    chunks = qr_sem.shape[1]
    chunk = share // chunks

    def rows_of(index, c):
        return q_ref.at[pl.ds(index * share + c * chunk, chunk)]

    for c in range(chunks):
        source = block_ref.at[pl.ds(c * chunk, chunk)]
        for i in range(1, high_count):
            peer = lax.rem(high + i, high_count) * LOW + low
            sends.append(send(source, rows_of(seq, c), qs_sem.at[i - 1, c], qr_sem.at[seq, c],
                              "seq", peer))
        sends.append(send(source, rows_of(seq, c), qs_sem.at[high_count - 1, c], qr_sem.at[seq, c],
                          "seq", pair))
    q_ref[pl.ds(seq * share, share)] = block_ref[...]
    for c in range(chunks):
        for i in range(1, high_count):
            block = lax.rem(high + high_count - i, high_count) * LOW + low
            arrived(rows_of(block, c), qr_sem.at[block, c])
            sends.append(send(rows_of(block, c), rows_of(block, c), qf_sem.at[i - 1, c],
                              qr_sem.at[block, c], "seq", pair))

    lane = lax.broadcasted_iota(jnp.int32, (share, HD), 1)
    for peer in range(n_seq):
        kv = peer * head_share // group_q
        scores = jnp.zeros((share, HD), jnp.float32)
        for k in range(head_share):
            head = peer * head_share + k
            key = head_rows(HQ + head // group_q)
            score = jnp.sum(head_rows(head) * key, axis=1, keepdims=True) * (HD**-0.5)
            scores = jnp.where(lane == k, score, scores)
        nv_send[peer, 0] = scores
        nv_send[peer, 1] = head_rows(HQ + KVH + kv)
    for i in range(1, n_seq):
        peer = lax.rem(seq + i, n_seq)
        sends.append(
            send(nv_send.at[peer], nv_ref.at[seq], ns_sem.at[i - 1], nr_sem.at[seq], "seq", peer)
        )
    nv_ref[seq] = nv_send[seq]
    stat_ref[...] = jnp.zeros_like(stat_ref)
    key_copy.wait()
    value_copy.wait()
    for h in range(high_count):
        for c in range(chunks):
            block = h * LOW + 1 - low
            arrived(rows_of(block, c), qr_sem.at[block, c])

    blocks, block_rows, _ = o_send.shape
    block_pages = block_rows // HQ
    pool_pages = blocks * block_pages
    unroll = math.gcd(block_pages, 8)
    place = lax.broadcasted_iota(jnp.int32, (HQ, PAGE), 1)
    spot = lax.broadcasted_iota(jnp.int32, (HQ, HD), 1)
    own_rows = head_share * block_pages

    def attend(first, step, carry):
        stat = stat_ref[...].reshape(HQ, HD)
        for j in range(unroll):
            within = step * unroll + j
            page = first + within
            alive = place < live_ref[page]
            query = q_ref[owner_ref[page]]
            start = pl.multiple_of(page * PAGE, PAGE)
            keys = key_ref[pl.ds(start, PAGE), :]
            values = value_ref[pl.ds(start, PAGE), :]
            scores = jnp.concatenate(
                [
                    lax.dot_general(
                        query[h * group_q : (h + 1) * group_q],
                        keys[:, h * HD : (h + 1) * HD],
                        (((1,), (1,)), ((), ())),
                        preferred_element_type=jnp.float32,
                    )
                    for h in range(KVH)
                ],
                axis=0,
            ) * (HD**-0.5)
            scores = jnp.where(alive, scores, neg_fill)
            page_max = jnp.max(scores, axis=1, keepdims=True)
            weights = jnp.where(alive, jnp.exp(scores - page_max), 0.0)
            page_total = jnp.sum(weights, axis=1, keepdims=True)
            rounded = weights.astype(jnp.bfloat16)
            page_out = jnp.concatenate(
                [
                    jnp.dot(
                        rounded[h * group_q : (h + 1) * group_q],
                        values[:, h * HD : (h + 1) * HD],
                        preferred_element_type=jnp.float32,
                    )
                    for h in range(KVH)
                ],
                axis=0,
            )
            page_ref[pl.ds(within, HQ, stride=block_pages), :] = page_out
            holder = jnp.where(live_ref[page] > 0, owner_ref[page], -1).astype(jnp.float32)
            stat = jnp.where(spot == page, page_max, stat)
            stat = jnp.where(spot == pool_pages + page, page_total, stat)
            stat = jnp.where(spot == 2 * pool_pages + page, holder, stat)
        stat_ref[...] = stat.reshape(stat_ref.shape)
        return carry

    for b in range(blocks):
        lax.fori_loop(
            0, block_pages // unroll, functools.partial(attend, b * block_pages), 0
        )
        o_send[b] = page_ref[...].astype(jnp.bfloat16)
        for i in range(1, n_seq):
            peer = lax.rem(seq + i, n_seq)
            if b == blocks - 1:
                sends.append(send(stat_ref.at[peer], s_all.at[seq], ss_sem.at[i - 1],
                                  sr_sem.at[seq], "seq", peer))
            sends.append(send(o_send.at[b, pl.ds(peer * own_rows, own_rows)], o_all.at[seq, b],
                              os_sem.at[i - 1, b], or_sem.at[seq, b], "seq", peer))
        o_all[seq, b] = o_send[b, pl.ds(pl.multiple_of(seq * own_rows, own_rows), own_rows)]
    s_all[seq] = stat_ref[seq]

    for i in range(1, n_seq):
        block = lax.rem(seq + i, n_seq)
        arrived(nv_ref.at[block], nr_sem.at[block])
        arrived(s_all.at[block], sr_sem.at[block])
    packed = HD // pool_pages
    slots = n_seq * pool_pages
    spot = lax.broadcasted_iota(jnp.int32, (head_share, HD), 1) // pool_pages

    def lined_up(field):
        tiles = []
        for first in range(0, n_seq, packed):
            tile = jnp.zeros((head_share, HD), jnp.float32)
            for k in range(packed):
                shift = (HD + (k - field) * pool_pages) % HD
                source = s_all[first + k]
                tile = jnp.where(spot == k, pltpu.roll(source, shift, 1) if shift else source, tile)
            tiles.append(tile)
        return jnp.concatenate(tiles, axis=1)

    tops, totals, holders = lined_up(0), lined_up(1), lined_up(2)
    request = lax.broadcasted_iota(jnp.int32, (group_size, slots), 0).astype(jnp.float32)
    held = request == holders[:1, :]
    fresh_scores = nv_ref[:, 0].reshape(group_size, HD)
    fresh_values = nv_ref[:, 1].reshape(group_size, HD)
    for b in range(blocks):
        for i in range(1, n_seq):
            block = lax.rem(seq + i, n_seq)
            arrived(o_all.at[block, b], or_sem.at[block, b])
    parts = att_all.shape[0]
    part_heads = head_share // parts
    part = part_heads * HD
    for a in range(parts):
        for m in range(part_heads):
            k = a * part_heads + m
            top = jnp.where(held, tops[k : k + 1, :], neg_fill)
            fresh = fresh_scores[:, k : k + 1]
            peak = jnp.maximum(jnp.max(top, axis=1, keepdims=True), fresh)
            factor = jnp.where(held, jnp.exp(top - peak), 0.0)
            fresh_weight = jnp.exp(fresh - peak)
            denominator = (
                jnp.sum(factor * totals[k : k + 1, :], axis=1, keepdims=True) + fresh_weight
            )
            coarse = factor.astype(jnp.bfloat16)
            fine = (factor - coarse.astype(jnp.float32)).astype(jnp.bfloat16)
            outs = o_all[:, :, k * block_pages : (k + 1) * block_pages, :].reshape(slots, HD)
            numerator = (
                jnp.dot(coarse, outs, preferred_element_type=jnp.float32)
                + jnp.dot(fine, outs, preferred_element_type=jnp.float32)
                + fresh_weight * fresh_values
            )
            att_ref[a, :, m * HD : (m + 1) * HD] = (numerator / denominator).astype(jnp.bfloat16)
        sends += gather_start(n_grp, att_ref.at[a], att_all.at[a], as_sem.at[a], ar_sem.at[a])
    for a in range(parts):
        sends += gather_relay(n_grp, att_all.at[a], as_sem.at[a], ar_sem.at[a])
    for a in range(parts):
        gather_finish(n_grp, att_all.at[a], ar_sem.at[a])
        rows_ref[:, a * part : (a + 1) * part] = jnp.dot(
            back_ref[...], att_all[a].reshape(-1, part), preferred_element_type=jnp.float32
        ).astype(jnp.bfloat16)

    def keep(p, total):
        mixed_ref[:, pl.ds(pl.multiple_of(p * out_width, out_width), out_width)] = total.astype(
            jnp.bfloat16
        )

    drain_out = reduce_scatter(n_seq, rows_ref.at[:, :out_depth], w_out_ref, out_fetch, m_own,
                               m_ys, m_yr, m_zs, m_zr, (m_ys_sem, m_yr_sem, m_zs_sem, m_zr_sem),
                               keep)
    drain_in()
    drain_out()
    for copy in sends:
        copy.wait_send()


def run_step(n_seq, n_grp, owner, live, hidden, perm, back, bias, cosine, sine, w_qkv, w_out,
             k_cache, v_cache):
    group_size, depth = hidden.shape
    request_total = perm.shape[0]
    in_cols = w_qkv.shape[1]
    out_depth, out_cols = w_out.shape
    in_pieces, out_pieces = math.gcd(in_cols // HD, 10), math.gcd(out_cols // HD, 8)
    in_width, out_width = in_cols // in_pieces, out_cols // out_pieces
    half = request_total // LOW
    high_count = n_seq // LOW
    row_share = half // high_count
    share = row_share // n_grp
    head_share = HQ // n_seq
    block_rows = share * in_cols // HD
    positions = k_cache.shape[1]
    pool_pages = positions // PAGE
    block_pages = math.gcd(pool_pages, 16)
    blocks = pool_pages // block_pages
    chunks = math.gcd(share, 4)
    parts = 2
    bf16, f32 = jnp.bfloat16, jnp.float32
    dma = pltpu.SemaphoreType.DMA
    vmem = pl.BlockSpec(memory_space=pltpu.VMEM)
    smem = pl.BlockSpec(memory_space=pltpu.SMEM)
    hbm = pl.BlockSpec(memory_space=pl.ANY)
    scratch = [
        ((positions, KVH * HD), bf16),
        ((positions, KVH * HD), bf16),
        ((in_pieces, depth, in_width), bf16),
        ((out_pieces, out_depth, out_width), bf16),
        ((parts, n_grp, group_size, depth // parts), bf16),
        ((request_total, max(depth, out_depth)), bf16),
        ((in_pieces, high_count, row_share, in_width), f32),
        ((in_pieces, half, in_width), f32),
        ((in_pieces, half, in_width), f32),
        ((in_pieces, high_count, row_share, in_width), f32),
        ((in_pieces, high_count - 1, row_share, in_width), f32),
        ((n_grp, block_rows, HD), f32),
        ((n_grp, block_rows, HD), bf16),
        ((n_grp - 1, block_rows, HD), bf16),
        ((n_grp, block_rows, HD), f32),
        ((share * HQ, HD), f32),
        ((share, HQ, HD), bf16),
        ((group_size, HQ, HD), bf16),
        ((n_seq, 2, share, HD), f32),
        ((n_seq, 2, share, HD), f32),
        ((HQ * block_pages, HD), f32),
        ((n_seq, head_share, HD), f32),
        ((blocks, HQ * block_pages, HD), bf16),
        ((n_seq, blocks, head_share * block_pages, HD), bf16),
        ((n_seq, head_share, HD), f32),
        ((parts, group_size, out_depth // parts), bf16),
        ((parts, n_grp, group_size, out_depth // parts), bf16),
        ((out_pieces, high_count, row_share, out_width), f32),
        ((out_pieces, half, out_width), bf16),
        ((out_pieces, half, out_width), bf16),
        ((out_pieces, high_count, row_share, out_width), bf16),
        ((out_pieces, high_count - 1, row_share, out_width), bf16),
    ]
    sems = [
        (in_pieces,), (out_pieces,), (2,), (parts, 2 * n_grp), (parts, n_grp),
        (in_pieces,), (in_pieces,), (in_pieces, high_count - 1), (in_pieces, high_count - 1),
        (n_grp - 1,), (n_grp - 1,), (high_count, chunks), (high_count - 1, chunks),
        (n_seq, chunks), (n_seq - 1,), (n_seq,), (n_seq - 1, blocks), (n_seq, blocks),
        (n_seq - 1,), (n_seq,), (parts, 2 * n_grp), (parts, n_grp),
        (out_pieces,), (out_pieces,), (out_pieces, high_count - 1), (out_pieces, high_count - 1),
    ]
    return pl.pallas_call(
        functools.partial(step_kernel, n_seq, n_grp),
        out_shape=jax.ShapeDtypeStruct((row_share, out_cols), bf16),
        in_specs=[smem, smem] + [vmem] * 6 + [hbm] * 4,
        out_specs=vmem,
        scratch_shapes=[pltpu.VMEM(s, t) for s, t in scratch] + [dma(s) for s in sems],
        compiler_params=pltpu.CompilerParams(
            collective_id=0, has_side_effects=True, vmem_limit_bytes=60 * 1024 * 1024
        ),
        cost_estimate=pl.CostEstimate(
            flops=2 * request_total * depth * in_cols,
            bytes_accessed=2 * depth * in_cols,
            transcendentals=0,
        ),
    )(owner, live, hidden, perm, back, bias, cosine, sine, w_qkv, w_out, k_cache, v_cache)


def rope_tables(places):
    freq_index = jnp.arange(HD // 2, dtype=jnp.int32)
    inverse_freq = jnp.exp(freq_index.astype(jnp.float32) * (-2.0 * math.log(rope_base) / HD))
    section = jnp.where(
        freq_index < HD // 8, 0, jnp.where(freq_index < HD // 8 + 3 * HD // 16, 1, 2)
    )
    place_float = places.astype(jnp.float32)
    chosen = jnp.where(
        section[None, :] == 0,
        place_float[0][:, None],
        jnp.where(section[None, :] == 1, place_float[1][:, None], place_float[2][:, None]),
    )
    angles = chosen * inverse_freq[None, :]
    cosine, sine = jnp.cos(angles), jnp.sin(angles)
    return jnp.concatenate([cosine, cosine], 1), jnp.concatenate([-sine, sine], 1)


def shards(hidden, w_qkv, b_qkv, w_out, k_cache, v_cache, lengths, page_table, positions, group_of):
    n_seq = lax.axis_size("seq")
    n_grp = lax.axis_size("grp")
    seq_index = lax.axis_index("seq")
    grp_index = lax.axis_index("grp")
    request_total = group_of.shape[0]
    group_size = request_total // n_grp
    share = group_size // n_seq
    high_count = n_seq // LOW
    row_share = request_total // n_seq
    request_ids = jnp.arange(request_total, dtype=jnp.int32)
    before = (group_of[None, :] < group_of[:, None]) | (group_of[None, :] == group_of[:, None]) & (
        request_ids[None, :] < request_ids[:, None]
    )
    served_at = jnp.sum(before.astype(jnp.int32), axis=1)
    rank = served_at % group_size
    holder = rank // share
    sent_at = (
        ((holder % LOW) * high_count + holder // LOW) * n_grp + served_at // group_size
    ) * share + rank % share
    in_perm = sent_at[None, :] == request_ids[:, None]
    my_start = ((seq_index % LOW) * high_count + seq_index // LOW) * row_share
    my_rows = (
        my_start + jnp.arange(row_share, dtype=jnp.int32)[:, None] == sent_at[None, :]
    )
    places = jnp.sum(jnp.where(my_rows[None], positions[:, None, :], 0), axis=2)
    cosine, sine = rope_tables(places)
    placed_at = served_at[None, :] == request_ids[:, None]
    served_order = jnp.sum(jnp.where(placed_at, request_ids[None, :], 0), axis=1)
    served_ids = lax.dynamic_slice_in_dim(served_order, grp_index * group_size, group_size, 0)
    served_len = lengths[served_ids]
    served_table = page_table[served_ids]
    most_pages = page_table.shape[1]
    page_counts = (served_len + PAGE - 1) // PAGE
    logical = jnp.arange(most_pages, dtype=jnp.int32)
    pool_pages = k_cache.shape[1] // PAGE
    local_page = served_table - seq_index * pool_pages
    usable = (
        (logical[None, :] < page_counts[:, None]) & (local_page >= 0) & (local_page < pool_pages)
    )
    pool_ids = jnp.arange(pool_pages, dtype=jnp.int32)
    matched = usable[:, :, None] & (local_page[:, :, None] == pool_ids[None, None, :])
    owner_ids = jnp.arange(group_size, dtype=jnp.int32)
    left = served_len[:, None] - logical[None, :] * PAGE
    live = jnp.max(jnp.where(matched, left[:, :, None], 0), axis=(0, 1))
    owner = jnp.max(jnp.where(matched, owner_ids[:, None, None], 0), axis=(0, 1))
    back_at = served_at.reshape(high_count, LOW, row_share).transpose(1, 0, 2).reshape(-1)
    out_perm = back_at[:, None] == request_ids[None, :]
    return run_step(
        n_seq, n_grp, owner, live, hidden, in_perm.astype(jnp.bfloat16),
        out_perm.astype(jnp.bfloat16), b_qkv.reshape(-1, HD), cosine, sine, w_qkv, w_out, k_cache,
        v_cache
    )


def solution(mesh):
    placed = (
        P("grp", "seq"),
        P("seq", "grp"),
        P("grp"),
        P("seq", "grp"),
        P("grp", "seq", None),
        P("grp", "seq", None),
        P(),
        P(),
        P(),
        P(),
    )
    return jax.shard_map(
        shards, mesh=mesh, in_specs=placed, out_specs=P("seq", "grp"), check_vma=False
    )
```

```python
import functools
import math

import jax
import jax.numpy as jnp
from jax import lax
from jax.experimental import pallas as pl
from jax.experimental.pallas import tpu as pltpu
from jax.sharding import PartitionSpec as P

HQ = 64
KVH = 8
HD = 128
PAGE = 128
LOW = 2
MESH = pl.DeviceIdType.MESH

rope_base = 1000000.0
neg_fill = -1e30


def greet(n_seq, n_grp):
    seq, grp = lax.axis_index("seq"), lax.axis_index("grp")
    barrier = pltpu.get_barrier_semaphore()
    for i in range(1, n_seq):
        pl.semaphore_signal(
            barrier, inc=1, device_id={"seq": lax.rem(seq + i, n_seq)}, device_id_type=MESH
        )
    for i in range(1, n_grp):
        pl.semaphore_signal(
            barrier, inc=1, device_id={"grp": lax.rem(grp + i, n_grp)}, device_id_type=MESH
        )


def greeted(n_seq, n_grp):
    pl.semaphore_wait(pltpu.get_barrier_semaphore(), n_seq + n_grp - 2)


def split_exact(values):
    terms = []
    for _ in range(3):
        terms.append(values.astype(jnp.bfloat16))
        values = values - terms[-1].astype(jnp.float32)
    return terms


def row_col(shape):
    return tuple(lax.broadcasted_iota(jnp.int32, shape, d).astype(jnp.float32) for d in (0, 1))


def one_hot(mask):
    return mask.astype(jnp.float32).astype(jnp.bfloat16)


def whole_part(values, divisor):
    return jnp.floor((values + 0.5) * (1.0 / divisor))


def serve_order(n_seq, n_grp, group_of_ref, perm_ref):
    total = group_of_ref.shape[1]
    group_size = total // n_grp
    share = group_size // n_seq
    row, col = row_col((total, total))
    member = group_of_ref[...].astype(jnp.float32)
    member_down = jnp.sum(jnp.where(row == col, member, 0.0), axis=1, keepdims=True)
    earlier = (member_down < member) | ((member_down == member) & (row < col))
    served = jnp.sum(jnp.where(earlier, 1.0, 0.0), axis=0, keepdims=True)
    rank = served - member * group_size
    holder = whole_part(rank, share)
    high = whole_part(holder, LOW)
    low = holder - high * LOW
    sent = ((low * (n_seq // LOW) + high) * n_grp + member) * share + rank - holder * share
    perm_ref[...] = one_hot(row == sent)
    return served, sent


def serve_tables(n_seq, n_grp, order, group_of_ref, len_ref, table_ref, cos_all_ref, sin_all_ref, back_ref,
                 cos_ref, sin_ref, slot_ref):
    served, sent = order
    seq, grp = lax.axis_index("seq"), lax.axis_index("grp")
    total = served.shape[1]
    group_size = total // n_grp
    row_share = total // n_seq
    high_count = n_seq // LOW
    pool_pages = slot_ref.shape[0]
    row, col = row_col((total, total))
    low_part = whole_part(row, total // LOW)
    rest = row - low_part * (total // LOW)
    high_part = whole_part(rest, row_share)
    wanted = (high_part * LOW + low_part) * row_share + rest - high_part * row_share
    served_down = jnp.sum(jnp.where(col == wanted, served, 0.0), axis=1, keepdims=True)
    back_ref[...] = one_hot(col == served_down)

    start = (lax.rem(seq, LOW) * high_count + seq // LOW) * row_share
    row, _ = row_col((row_share, total))
    mine = one_hot(row + start.astype(jnp.float32) == sent)
    for source, target in ((cos_all_ref, cos_ref), (sin_all_ref, sin_ref)):
        target[...] = sum(
            jnp.dot(mine, term, preferred_element_type=jnp.float32)
            for term in split_exact(source[...])
        )

    row = lax.broadcasted_iota(jnp.int32, (total, total), 0)
    col = lax.broadcasted_iota(jnp.int32, (total, total), 1)
    member = group_of_ref[...]
    member_down = jnp.sum(jnp.where(row == col, member, 0), axis=1, keepdims=True)
    lengths = jnp.sum(jnp.where(row == col, len_ref[...], 0), axis=1, keepdims=True)
    earlier = (member < member_down) | ((member == member_down) & (col < row))
    rank_down = jnp.sum(jnp.where(earlier, 1, 0), axis=1, keepdims=True) - member_down * group_size
    place = table_ref[...] - seq * pool_pages
    left = lengths - lax.broadcasted_iota(jnp.int32, place.shape, 1) * PAGE
    code = jnp.where((member_down == grp) & (left > 0), left * group_size + rank_down, 0)
    codes = jnp.concatenate(
        [
            jnp.sum(jnp.where(place == p, code, 0), axis=0, keepdims=True)
            for p in range(pool_pages)
        ],
        axis=0,
    )
    slot_ref[...] = jnp.broadcast_to(jnp.sum(codes, axis=1, keepdims=True), slot_ref.shape)


def send(src, dst, send_sem, recv_sem, axis, index):
    copy = pltpu.make_async_remote_copy(
        src_ref=src,
        dst_ref=dst,
        send_sem=send_sem,
        recv_sem=recv_sem,
        device_id={axis: index},
        device_id_type=MESH,
    )
    copy.start()
    return copy


def arrived(ref, sem):
    pltpu.make_async_copy(ref, ref, sem).wait()


def gather_start(n_grp, own_ref, all_ref, send_sem, recv_sem):
    grp = lax.axis_index("grp")
    high_count = n_grp // LOW
    high, low = grp // LOW, lax.rem(grp, LOW)
    copies = [
        send(own_ref, all_ref.at[grp], send_sem.at[i - 1], recv_sem.at[grp], "grp",
             lax.rem(high + i, high_count) * LOW + low)
        for i in range(1, high_count)
    ]
    copies.append(
        send(own_ref, all_ref.at[grp], send_sem.at[high_count - 1], recv_sem.at[grp], "grp",
             grp + 1 - 2 * low)
    )
    all_ref[grp] = own_ref[...]
    return copies


def gather_relay(n_grp, all_ref, send_sem, recv_sem):
    grp = lax.axis_index("grp")
    high_count = n_grp // LOW
    high, low = grp // LOW, lax.rem(grp, LOW)
    copies = []
    for i in range(1, high_count):
        block = lax.rem(high + high_count - i, high_count) * LOW + low
        arrived(all_ref.at[block], recv_sem.at[block])
        copies.append(
            send(all_ref.at[block], all_ref.at[block], send_sem.at[high_count - 1 + i],
                 recv_sem.at[block], "grp", grp + 1 - 2 * low)
        )
    return copies


def gather_finish(n_grp, all_ref, recv_sem):
    low = lax.rem(lax.axis_index("grp"), LOW)
    for h in range(n_grp // LOW):
        block = h * LOW + 1 - low
        arrived(all_ref.at[block], recv_sem.at[block])


def reduce_scatter(n_seq, rows_ref, w_ref, fetch, own_ref, y_send, y_recv, z_send, z_recv, sems,
                   finish, lag):
    ys_sem, yr_sem, zs_sem, zr_sem = sems
    pieces, _, width = w_ref.shape
    seq = lax.axis_index("seq")
    high_count = n_seq // LOW
    high, low = seq // LOW, lax.rem(seq, LOW)
    half = rows_ref.shape[0] // LOW
    row_share = half // high_count
    wire = y_send.dtype

    def y_copy(p):
        return pltpu.make_async_remote_copy(
            src_ref=y_send.at[p], dst_ref=y_recv.at[p], send_sem=ys_sem.at[p],
            recv_sem=yr_sem.at[p], device_id={"seq": seq + 1 - 2 * low}, device_id_type=MESH)

    def z_copy(p, i):
        peer = lax.rem(high + i, high_count)
        return pltpu.make_async_remote_copy(
            src_ref=z_send.at[p, peer], dst_ref=z_recv.at[p, i - 1], send_sem=zs_sem.at[p, i - 1],
            recv_sem=zr_sem.at[p, i - 1], device_id={"seq": peer * LOW + low},
            device_id_type=MESH)

    def multiply(p, carry):
        fetch(p).wait()
        theirs = rows_ref[pl.ds(pl.multiple_of((1 - low) * half, half), half), :]
        y_send[p] = jnp.dot(theirs, w_ref[p], preferred_element_type=jnp.float32).astype(wire)
        y_copy(p).start()
        mine = rows_ref[pl.ds(pl.multiple_of(low * half, half), half), :]
        own_ref[p] = jnp.dot(mine, w_ref[p], preferred_element_type=jnp.float32).reshape(
            high_count, row_share, width
        )
        return carry

    def spread(p):
        y_copy(p).wait_recv()
        summed = own_ref[p] + y_recv[p].astype(jnp.float32).reshape(high_count, row_share, width)
        own_ref[p] = summed
        z_send[p] = summed.astype(wire)
        for i in range(1, high_count):
            z_copy(p, i).start()

    def collect(p):
        total = own_ref[p, high]
        for i in range(1, high_count):
            z_copy(p, i).wait_recv()
            total = total + z_recv[p, i - 1].astype(jnp.float32)
        finish(p, total)

    def first(p, carry):
        spread(p)
        return carry

    def step(p, carry):
        spread(p)
        collect(p - lag)
        return carry

    def last(p, carry):
        collect(p)
        return carry

    def drain(p, carry):
        y_copy(p).wait_send()
        for i in range(1, high_count):
            z_copy(p, i).wait_send()
        return carry

    lax.fori_loop(0, pieces, multiply, 0)
    lag = min(lag, pieces)
    lax.fori_loop(0, lag, first, 0)
    lax.fori_loop(lag, pieces, step, 0)
    lax.fori_loop(pieces - lag, pieces, last, 0)
    return lambda: lax.fori_loop(0, pieces, drain, 0)


def step_kernel(n_seq, n_grp, hidden_ref, group_of_ref, len_ref, table_ref, bias_ref,
                cos_all_ref, sin_all_ref, w_in_hbm, w_out_hbm, k_hbm, v_hbm, mixed_ref,
                perm_ref, back_ref, cos_ref, sin_ref, slot_ref, slots_ref,
                key_ref, value_ref, w_in_ref, w_out_ref, hid_all, rows_ref, p_own, p_ys, p_yr,
                p_zs, p_zr, turned_ref, d_send, d_recv, x_ref, wide_ref, block_ref, q_ref, nv_send,
                nv_ref, page_ref, stat_ref, o_send, o_all, s_all, att_ref, att_all, m_own, m_ys,
                m_yr, m_zs, m_zr, slot_sem, w_in_sem, w_out_sem, kv_sem, hs_sem, hr_sem, p_ys_sem, p_yr_sem,
                p_zs_sem, p_zr_sem, ds_sem, dr_sem, qs_sem, qf_sem, qr_sem, ns_sem, nr_sem, os_sem,
                or_sem, ss_sem, sr_sem, as_sem, ar_sem, m_ys_sem, m_yr_sem, m_zs_sem, m_zr_sem):
    seq, grp = lax.axis_index("seq"), lax.axis_index("grp")
    high_count = n_seq // LOW
    high, low = seq // LOW, lax.rem(seq, LOW)
    pair = seq + 1 - 2 * low
    in_pieces, depth, in_width = w_in_ref.shape
    out_pieces, out_depth, out_width = w_out_ref.shape
    parts = hid_all.shape[0]
    share = block_ref.shape[0]
    piece_heads = in_width // HD
    block_heads = in_pieces * piece_heads
    head_share = HQ // n_seq
    group_q = HQ // KVH
    group_size = share * n_seq

    def in_fetch(p):
        return pltpu.make_async_copy(
            w_in_hbm.at[:, pl.ds(pl.multiple_of(p * in_width, in_width), in_width)],
            w_in_ref.at[p], w_in_sem.at[p])

    def out_fetch(p):
        return pltpu.make_async_copy(
            w_out_hbm.at[:, pl.ds(pl.multiple_of(p * out_width, out_width), out_width)],
            w_out_ref.at[p], w_out_sem.at[p])

    key_copy = pltpu.make_async_copy(k_hbm.at[0], key_ref, kv_sem.at[0])
    value_copy = pltpu.make_async_copy(v_hbm.at[0], value_ref, kv_sem.at[1])
    for p in range(in_pieces):
        in_fetch(p).start()
    greet(n_seq, n_grp)
    order = serve_order(n_seq, n_grp, group_of_ref, perm_ref)
    greeted(n_seq, n_grp)

    sends = []
    part = depth // parts
    for a in range(parts):
        sends += gather_start(n_grp, hidden_ref.at[:, a * part : (a + 1) * part], hid_all.at[a],
                              hs_sem.at[a], hr_sem.at[a])
    key_copy.start()
    value_copy.start()
    for p in range(out_pieces):
        out_fetch(p).start()
    serve_tables(n_seq, n_grp, order, group_of_ref, len_ref, table_ref, cos_all_ref, sin_all_ref, back_ref,
                 cos_ref, sin_ref, slot_ref)
    slot_copy = pltpu.make_async_copy(slot_ref, slots_ref, slot_sem)
    slot_copy.start()
    for a in range(parts):
        sends += gather_relay(n_grp, hid_all.at[a], hs_sem.at[a], hr_sem.at[a])
    for a in range(parts):
        gather_finish(n_grp, hid_all.at[a], hr_sem.at[a])
        rows_ref[:, a * part : (a + 1) * part] = jnp.dot(
            perm_ref[...], hid_all[a].reshape(-1, part), preferred_element_type=jnp.float32
        ).astype(jnp.bfloat16)

    def turn(p, total):
        for k in range(piece_heads):
            head = p * piece_heads + k
            values = total[:, k * HD : (k + 1) * HD] + bias_ref[pl.ds(head, 1), :]
            rotated = values * cos_ref[...] + pltpu.roll(values, HD // 2, 1) * sin_ref[...]
            values = jnp.where(grp * block_heads + head < HQ + KVH, rotated, values)
            for g in range(n_grp):
                turned_ref[g, pl.ds(head, share, stride=block_heads), :] = values[
                    g * share : (g + 1) * share
                ]

    drain_in = reduce_scatter(n_seq, rows_ref, w_in_ref, in_fetch, p_own, p_ys, p_yr, p_zs, p_zr,
                              (p_ys_sem, p_yr_sem, p_zs_sem, p_zr_sem), turn, 2)

    d_send[...] = turned_ref[...].astype(jnp.bfloat16)
    head_sends = []
    for i in range(1, n_grp):
        peer = lax.rem(grp + i, n_grp)
        head_sends.append(
            send(d_send.at[peer], d_recv.at[i - 1], ds_sem.at[i - 1], dr_sem.at[i - 1], "grp", peer)
        )
    x_ref[grp] = d_send[grp].astype(jnp.float32)
    for i in range(1, n_grp):
        head_sends[i - 1].wait_recv()
        x_ref[lax.rem(grp + n_grp - i, n_grp)] = d_recv[i - 1].astype(jnp.float32)
    sends += head_sends

    def head_rows(head):
        return x_ref[head // block_heads, pl.ds(head % block_heads, share, stride=block_heads), :]

    for head in range(HQ):
        wide_ref[pl.ds(head, share, stride=HQ), :] = head_rows(head)
    block_ref[...] = wide_ref[...].reshape(share, HQ, HD).astype(jnp.bfloat16)

    chunks = qr_sem.shape[1]
    chunk = share // chunks

    def rows_of(index, c):
        return q_ref.at[pl.ds(index * share + c * chunk, chunk)]

    for c in range(chunks):
        source = block_ref.at[pl.ds(c * chunk, chunk)]
        for i in range(1, high_count):
            peer = lax.rem(high + i, high_count) * LOW + low
            sends.append(send(source, rows_of(seq, c), qs_sem.at[i - 1, c], qr_sem.at[seq, c],
                              "seq", peer))
        sends.append(send(source, rows_of(seq, c), qs_sem.at[high_count - 1, c], qr_sem.at[seq, c],
                          "seq", pair))
    q_ref[pl.ds(seq * share, share)] = block_ref[...]
    for c in range(chunks):
        for i in range(1, high_count):
            block = lax.rem(high + high_count - i, high_count) * LOW + low
            arrived(rows_of(block, c), qr_sem.at[block, c])
            sends.append(send(rows_of(block, c), rows_of(block, c), qf_sem.at[i - 1, c],
                              qr_sem.at[block, c], "seq", pair))

    lane = lax.broadcasted_iota(jnp.int32, (share, HD), 1)
    for peer in range(n_seq):
        kv = peer * head_share // group_q
        scores = jnp.zeros((share, HD), jnp.float32)
        for k in range(head_share):
            head = peer * head_share + k
            key = head_rows(HQ + head // group_q)
            score = jnp.sum(head_rows(head) * key, axis=1, keepdims=True) * (HD**-0.5)
            scores = jnp.where(lane == k, score, scores)
        nv_send[peer, 0] = scores
        nv_send[peer, 1] = head_rows(HQ + KVH + kv)
    for i in range(1, n_seq):
        peer = lax.rem(seq + i, n_seq)
        sends.append(
            send(nv_send.at[peer], nv_ref.at[seq], ns_sem.at[i - 1], nr_sem.at[seq], "seq", peer)
        )
    nv_ref[seq] = nv_send[seq]
    stat_ref[...] = jnp.zeros_like(stat_ref)
    slot_copy.wait()
    key_copy.wait()
    value_copy.wait()
    for h in range(high_count):
        for c in range(chunks):
            block = h * LOW + 1 - low
            arrived(rows_of(block, c), qr_sem.at[block, c])

    blocks, block_rows, _ = o_send.shape
    block_pages = block_rows // HQ
    pool_pages = blocks * block_pages
    unroll = math.gcd(block_pages, 8)
    place = lax.broadcasted_iota(jnp.int32, (HQ, PAGE), 1)
    spot = lax.broadcasted_iota(jnp.int32, (HQ, HD), 1)
    own_rows = head_share * block_pages

    def attend(first, step, carry):
        stat = stat_ref[...].reshape(HQ, HD)
        for j in range(unroll):
            within = step * unroll + j
            page = first + within
            page_live, owner = slots_ref[page, 0] // group_size, slots_ref[page, 0] % group_size
            alive = place < page_live
            query = q_ref[owner]
            start = pl.multiple_of(page * PAGE, PAGE)
            keys = key_ref[pl.ds(start, PAGE), :]
            values = value_ref[pl.ds(start, PAGE), :]
            scores = jnp.concatenate(
                [
                    lax.dot_general(
                        query[h * group_q : (h + 1) * group_q],
                        keys[:, h * HD : (h + 1) * HD],
                        (((1,), (1,)), ((), ())),
                        preferred_element_type=jnp.float32,
                    )
                    for h in range(KVH)
                ],
                axis=0,
            ) * (HD**-0.5)
            scores = jnp.where(alive, scores, neg_fill)
            page_max = jnp.max(scores, axis=1, keepdims=True)
            weights = jnp.where(alive, jnp.exp(scores - page_max), 0.0)
            page_total = jnp.sum(weights, axis=1, keepdims=True)
            rounded = weights.astype(jnp.bfloat16)
            page_out = jnp.concatenate(
                [
                    jnp.dot(
                        rounded[h * group_q : (h + 1) * group_q],
                        values[:, h * HD : (h + 1) * HD],
                        preferred_element_type=jnp.float32,
                    )
                    for h in range(KVH)
                ],
                axis=0,
            )
            page_ref[pl.ds(within, HQ, stride=block_pages), :] = page_out
            holder = jnp.where(page_live > 0, owner, -1).astype(jnp.float32)
            stat = jnp.where(spot == page, page_max, stat)
            stat = jnp.where(spot == pool_pages + page, page_total, stat)
            stat = jnp.where(spot == 2 * pool_pages + page, holder, stat)
        stat_ref[...] = stat.reshape(stat_ref.shape)
        return carry

    for b in range(blocks):
        lax.fori_loop(
            0, block_pages // unroll, functools.partial(attend, b * block_pages), 0
        )
        o_send[b] = page_ref[...].astype(jnp.bfloat16)
        for i in range(1, n_seq):
            peer = lax.rem(seq + i, n_seq)
            if b == blocks - 1:
                sends.append(send(stat_ref.at[peer], s_all.at[seq], ss_sem.at[i - 1],
                                  sr_sem.at[seq], "seq", peer))
            sends.append(send(o_send.at[b, pl.ds(peer * own_rows, own_rows)], o_all.at[seq, b],
                              os_sem.at[i - 1, b], or_sem.at[seq, b], "seq", peer))
        o_all[seq, b] = o_send[b, pl.ds(pl.multiple_of(seq * own_rows, own_rows), own_rows)]
    s_all[seq] = stat_ref[seq]

    for i in range(1, n_seq):
        block = lax.rem(seq + i, n_seq)
        arrived(nv_ref.at[block], nr_sem.at[block])
        arrived(s_all.at[block], sr_sem.at[block])
    packed = HD // pool_pages
    slots = n_seq * pool_pages
    spot = lax.broadcasted_iota(jnp.int32, (head_share, HD), 1) // pool_pages

    def lined_up(field):
        tiles = []
        for first in range(0, n_seq, packed):
            tile = jnp.zeros((head_share, HD), jnp.float32)
            for k in range(packed):
                shift = (HD + (k - field) * pool_pages) % HD
                source = s_all[first + k]
                tile = jnp.where(spot == k, pltpu.roll(source, shift, 1) if shift else source, tile)
            tiles.append(tile)
        return jnp.concatenate(tiles, axis=1)

    tops, totals, holders = lined_up(0), lined_up(1), lined_up(2)
    request = lax.broadcasted_iota(jnp.int32, (group_size, slots), 0).astype(jnp.float32)
    held = request == holders[:1, :]
    fresh_scores = nv_ref[:, 0].reshape(group_size, HD)
    fresh_values = nv_ref[:, 1].reshape(group_size, HD)
    for b in range(blocks):
        for i in range(1, n_seq):
            block = lax.rem(seq + i, n_seq)
            arrived(o_all.at[block, b], or_sem.at[block, b])
    parts = att_all.shape[0]
    part_heads = head_share // parts
    part = part_heads * HD
    for a in range(parts):
        for m in range(part_heads):
            k = a * part_heads + m
            top = jnp.where(held, tops[k : k + 1, :], neg_fill)
            fresh = fresh_scores[:, k : k + 1]
            peak = jnp.maximum(jnp.max(top, axis=1, keepdims=True), fresh)
            factor = jnp.where(held, jnp.exp(top - peak), 0.0)
            fresh_weight = jnp.exp(fresh - peak)
            denominator = (
                jnp.sum(factor * totals[k : k + 1, :], axis=1, keepdims=True) + fresh_weight
            )
            coarse = factor.astype(jnp.bfloat16)
            fine = (factor - coarse.astype(jnp.float32)).astype(jnp.bfloat16)
            outs = o_all[:, :, k * block_pages : (k + 1) * block_pages, :].reshape(slots, HD)
            numerator = (
                jnp.dot(coarse, outs, preferred_element_type=jnp.float32)
                + jnp.dot(fine, outs, preferred_element_type=jnp.float32)
                + fresh_weight * fresh_values
            )
            att_ref[a, :, m * HD : (m + 1) * HD] = (numerator / denominator).astype(jnp.bfloat16)
        sends += gather_start(n_grp, att_ref.at[a], att_all.at[a], as_sem.at[a], ar_sem.at[a])
    for a in range(parts):
        sends += gather_relay(n_grp, att_all.at[a], as_sem.at[a], ar_sem.at[a])
    for a in range(parts):
        gather_finish(n_grp, att_all.at[a], ar_sem.at[a])
        rows_ref[:, a * part : (a + 1) * part] = jnp.dot(
            back_ref[...], att_all[a].reshape(-1, part), preferred_element_type=jnp.float32
        ).astype(jnp.bfloat16)

    def keep(p, total):
        mixed_ref[:, pl.ds(pl.multiple_of(p * out_width, out_width), out_width)] = total.astype(
            jnp.bfloat16
        )

    drain_out = reduce_scatter(n_seq, rows_ref.at[:, :out_depth], w_out_ref, out_fetch, m_own,
                               m_ys, m_yr, m_zs, m_zr, (m_ys_sem, m_yr_sem, m_zs_sem, m_zr_sem),
                               keep, 8)
    drain_in()
    drain_out()
    for copy in sends:
        copy.wait_send()


def run_step(n_seq, n_grp, hidden, group_of, lengths, table, bias, cosine, sine, w_qkv, w_out,
             k_cache, v_cache):
    group_size, depth = hidden.shape
    request_total = table.shape[0]
    in_cols = w_qkv.shape[1]
    out_depth, out_cols = w_out.shape
    in_pieces, out_pieces = math.gcd(in_cols // HD, 10), math.gcd(out_cols // HD, 8)
    in_width, out_width = in_cols // in_pieces, out_cols // out_pieces
    half = request_total // LOW
    high_count = n_seq // LOW
    row_share = half // high_count
    share = row_share // n_grp
    head_share = HQ // n_seq
    block_rows = share * in_cols // HD
    positions = k_cache.shape[1]
    pool_pages = positions // PAGE
    block_pages = math.gcd(pool_pages, 8)
    blocks = pool_pages // block_pages
    chunks = math.gcd(share, 4)
    parts = 2
    bf16, f32 = jnp.bfloat16, jnp.float32
    dma = pltpu.SemaphoreType.DMA
    vmem = pl.BlockSpec(memory_space=pltpu.VMEM)
    hbm = pl.BlockSpec(memory_space=pl.ANY)
    scratch = [
        ((request_total, request_total), bf16),
        ((request_total, request_total), bf16),
        ((row_share, HD), f32),
        ((row_share, HD), f32),
        ((pool_pages, HD), jnp.int32),
    ]
    smem_scratch = [pltpu.SMEM((pool_pages, HD), jnp.int32)]
    more_scratch = [
        ((positions, KVH * HD), bf16),
        ((positions, KVH * HD), bf16),
        ((in_pieces, depth, in_width), bf16),
        ((out_pieces, out_depth, out_width), bf16),
        ((parts, n_grp, group_size, depth // parts), bf16),
        ((request_total, max(depth, out_depth)), bf16),
        ((in_pieces, high_count, row_share, in_width), f32),
        ((in_pieces, half, in_width), f32),
        ((in_pieces, half, in_width), f32),
        ((in_pieces, high_count, row_share, in_width), f32),
        ((in_pieces, high_count - 1, row_share, in_width), f32),
        ((n_grp, block_rows, HD), f32),
        ((n_grp, block_rows, HD), bf16),
        ((n_grp - 1, block_rows, HD), bf16),
        ((n_grp, block_rows, HD), f32),
        ((share * HQ, HD), f32),
        ((share, HQ, HD), bf16),
        ((group_size, HQ, HD), bf16),
        ((n_seq, 2, share, HD), f32),
        ((n_seq, 2, share, HD), f32),
        ((HQ * block_pages, HD), f32),
        ((n_seq, head_share, HD), f32),
        ((blocks, HQ * block_pages, HD), bf16),
        ((n_seq, blocks, head_share * block_pages, HD), bf16),
        ((n_seq, head_share, HD), f32),
        ((parts, group_size, out_depth // parts), bf16),
        ((parts, n_grp, group_size, out_depth // parts), bf16),
        ((out_pieces, high_count, row_share, out_width), f32),
        ((out_pieces, half, out_width), bf16),
        ((out_pieces, half, out_width), bf16),
        ((out_pieces, high_count, row_share, out_width), bf16),
        ((out_pieces, high_count - 1, row_share, out_width), bf16),
    ]
    sems = [
        (in_pieces,), (out_pieces,), (2,), (parts, 2 * n_grp), (parts, n_grp),
        (in_pieces,), (in_pieces,), (in_pieces, high_count - 1), (in_pieces, high_count - 1),
        (n_grp - 1,), (n_grp - 1,), (high_count, chunks), (high_count - 1, chunks),
        (n_seq, chunks), (n_seq - 1,), (n_seq,), (n_seq - 1, blocks), (n_seq, blocks),
        (n_seq - 1,), (n_seq,), (parts, 2 * n_grp), (parts, n_grp),
        (out_pieces,), (out_pieces,), (out_pieces, high_count - 1), (out_pieces, high_count - 1),
    ]
    return pl.pallas_call(
        functools.partial(step_kernel, n_seq, n_grp),
        out_shape=jax.ShapeDtypeStruct((row_share, out_cols), bf16),
        in_specs=[vmem] * 7 + [hbm] * 4,
        out_specs=vmem,
        scratch_shapes=[pltpu.VMEM(s, t) for s, t in scratch]
        + smem_scratch
        + [pltpu.VMEM(s, t) for s, t in more_scratch]
        + [dma(())]
        + [dma(s) for s in sems],
        compiler_params=pltpu.CompilerParams(
            collective_id=0, has_side_effects=True, vmem_limit_bytes=60 * 1024 * 1024
        ),
        cost_estimate=pl.CostEstimate(
            flops=2 * request_total * depth * in_cols,
            bytes_accessed=2 * depth * in_cols,
            transcendentals=0,
        ),
    )(hidden, group_of, lengths, table, bias, cosine, sine, w_qkv, w_out, k_cache, v_cache)


def rope_tables(positions):
    column = jnp.arange(HD, dtype=jnp.int32)
    freq_index = column % (HD // 2)
    inverse_freq = jnp.exp(freq_index.astype(jnp.float32) * (-2.0 * math.log(rope_base) / HD))
    section = jnp.where(
        freq_index < HD // 8, 0, jnp.where(freq_index < HD // 8 + 3 * HD // 16, 1, 2)
    )
    place_float = positions.astype(jnp.float32)
    chosen = jnp.where(
        section[None, :] == 0,
        place_float[0][:, None],
        jnp.where(section[None, :] == 1, place_float[1][:, None], place_float[2][:, None]),
    )
    angles = chosen * inverse_freq[None, :]
    sine = jnp.sin(angles)
    return jnp.cos(angles), jnp.where((column < HD // 2)[None, :], -sine, sine)


def shards(hidden, w_qkv, b_qkv, w_out, k_cache, v_cache, lengths, page_table, positions, group_of):
    n_seq, n_grp = lax.axis_size("seq"), lax.axis_size("grp")
    cosine, sine = rope_tables(positions)
    return run_step(
        n_seq, n_grp, hidden, group_of[None, :], lengths[None, :], page_table,
        b_qkv.reshape(-1, HD), cosine, sine, w_qkv, w_out, k_cache, v_cache
    )


def solution(mesh):
    placed = (
        P("grp", "seq"),
        P("seq", "grp"),
        P("grp"),
        P("seq", "grp"),
        P("grp", "seq", None),
        P("grp", "seq", None),
        P(),
        P(),
        P(),
        P(),
    )
    return jax.shard_map(
        shards, mesh=mesh, in_specs=placed, out_specs=P("seq", "grp"), check_vma=False
    )
```

```python
import functools
import math

import jax
import jax.numpy as jnp
from jax import lax
from jax.experimental import pallas as pl
from jax.experimental.pallas import tpu as pltpu
from jax.sharding import PartitionSpec as P

HQ = 64
KVH = 8
HD = 128
PAGE = 128
LOW = 2
MESH = pl.DeviceIdType.MESH

rope_base = 1000000.0
neg_fill = -1e30


def greet(n_seq, n_grp):
    seq, grp = lax.axis_index("seq"), lax.axis_index("grp")
    barrier = pltpu.get_barrier_semaphore()
    for i in range(1, n_seq):
        pl.semaphore_signal(
            barrier, inc=1, device_id={"seq": lax.rem(seq + i, n_seq)}, device_id_type=MESH
        )
    for i in range(1, n_grp):
        pl.semaphore_signal(
            barrier, inc=1, device_id={"grp": lax.rem(grp + i, n_grp)}, device_id_type=MESH
        )


def greeted(n_seq, n_grp):
    pl.semaphore_wait(pltpu.get_barrier_semaphore(), n_seq + n_grp - 2)


def row_col(shape):
    return tuple(lax.broadcasted_iota(jnp.int32, shape, d).astype(jnp.float32) for d in (0, 1))


def one_hot(mask):
    return mask.astype(jnp.float32).astype(jnp.bfloat16)


def whole_part(values, divisor):
    return jnp.floor((values + 0.5) * (1.0 / divisor))


def serve_order(n_seq, n_grp, group_of_ref, perm_ref):
    total = group_of_ref.shape[1]
    group_size = total // n_grp
    share = group_size // n_seq
    row, col = row_col((total, total))
    member = group_of_ref[...].astype(jnp.float32)
    member_down = jnp.sum(jnp.where(row == col, member, 0.0), axis=1, keepdims=True)
    earlier = (member_down < member) | ((member_down == member) & (row < col))
    served = jnp.sum(jnp.where(earlier, 1.0, 0.0), axis=0, keepdims=True)
    rank = served - member * group_size
    holder = whole_part(rank, share)
    high = whole_part(holder, LOW)
    low = holder - high * LOW
    sent = ((low * (n_seq // LOW) + high) * n_grp + member) * share + rank - holder * share
    perm_ref[...] = one_hot(row == sent)
    return served, sent


def serve_tables(n_seq, n_grp, order, group_of_ref, len_ref, table_ref, place_ref, back_ref,
                 cos_ref, sin_ref, slot_ref):
    served, sent = order
    seq, grp = lax.axis_index("seq"), lax.axis_index("grp")
    total = served.shape[1]
    group_size = total // n_grp
    row_share = total // n_seq
    high_count = n_seq // LOW
    pool_pages = slot_ref.shape[0]
    row, col = row_col((total, total))
    low_part = whole_part(row, total // LOW)
    rest = row - low_part * (total // LOW)
    high_part = whole_part(rest, row_share)
    wanted = (high_part * LOW + low_part) * row_share + rest - high_part * row_share
    served_down = jnp.sum(jnp.where(col == wanted, served, 0.0), axis=1, keepdims=True)
    back_ref[...] = one_hot(col == served_down)

    start = (lax.rem(seq, LOW) * high_count + seq // LOW) * row_share
    row, _ = row_col((row_share, total))
    mine = row + start.astype(jnp.float32) == sent
    _, column = row_col((row_share, HD))
    freq_index = column - jnp.where(column < HD // 2, 0.0, HD // 2)
    inverse_freq = jnp.exp(freq_index * (-2.0 * math.log(rope_base) / HD))
    spots = [
        jnp.sum(
            jnp.where(mine, place_ref[k : k + 1, :].astype(jnp.float32), 0.0), axis=1, keepdims=True
        )
        for k in range(3)
    ]
    chosen = jnp.where(
        freq_index < HD // 8,
        spots[0],
        jnp.where(freq_index < HD // 8 + 3 * HD // 16, spots[1], spots[2]),
    )
    angles = chosen * inverse_freq
    sine = jnp.sin(angles)
    cos_ref[...] = jnp.cos(angles)
    sin_ref[...] = jnp.where(column < HD // 2, -sine, sine)

    row = lax.broadcasted_iota(jnp.int32, (total, total), 0)
    col = lax.broadcasted_iota(jnp.int32, (total, total), 1)
    member = group_of_ref[...]
    member_down = jnp.sum(jnp.where(row == col, member, 0), axis=1, keepdims=True)
    lengths = jnp.sum(jnp.where(row == col, len_ref[...], 0), axis=1, keepdims=True)
    earlier = (member < member_down) | ((member == member_down) & (col < row))
    rank_down = jnp.sum(jnp.where(earlier, 1, 0), axis=1, keepdims=True) - member_down * group_size
    place = table_ref[...] - seq * pool_pages
    left = lengths - lax.broadcasted_iota(jnp.int32, place.shape, 1) * PAGE
    code = jnp.where((member_down == grp) & (left > 0), left * group_size + rank_down, 0)
    codes = jnp.concatenate(
        [
            jnp.sum(jnp.where(place == p, code, 0), axis=0, keepdims=True)
            for p in range(pool_pages)
        ],
        axis=0,
    )
    slot_ref[...] = jnp.broadcast_to(jnp.sum(codes, axis=1, keepdims=True), slot_ref.shape)


def send(src, dst, send_sem, recv_sem, axis, index):
    copy = pltpu.make_async_remote_copy(
        src_ref=src,
        dst_ref=dst,
        send_sem=send_sem,
        recv_sem=recv_sem,
        device_id={axis: index},
        device_id_type=MESH,
    )
    copy.start()
    return copy


def arrived(ref, sem):
    pltpu.make_async_copy(ref, ref, sem).wait()


def gather_start(n_grp, own_ref, all_ref, send_sem, recv_sem):
    grp = lax.axis_index("grp")
    high_count = n_grp // LOW
    high, low = grp // LOW, lax.rem(grp, LOW)
    copies = [
        send(own_ref, all_ref.at[grp], send_sem.at[i - 1], recv_sem.at[grp], "grp",
             lax.rem(high + i, high_count) * LOW + low)
        for i in range(1, high_count)
    ]
    copies.append(
        send(own_ref, all_ref.at[grp], send_sem.at[high_count - 1], recv_sem.at[grp], "grp",
             grp + 1 - 2 * low)
    )
    all_ref[grp] = own_ref[...]
    return copies


def gather_relay(n_grp, all_ref, send_sem, recv_sem):
    grp = lax.axis_index("grp")
    high_count = n_grp // LOW
    high, low = grp // LOW, lax.rem(grp, LOW)
    copies = []
    for i in range(1, high_count):
        block = lax.rem(high + high_count - i, high_count) * LOW + low
        arrived(all_ref.at[block], recv_sem.at[block])
        copies.append(
            send(all_ref.at[block], all_ref.at[block], send_sem.at[high_count - 1 + i],
                 recv_sem.at[block], "grp", grp + 1 - 2 * low)
        )
    return copies


def gather_finish(n_grp, all_ref, recv_sem):
    low = lax.rem(lax.axis_index("grp"), LOW)
    for h in range(n_grp // LOW):
        block = h * LOW + 1 - low
        arrived(all_ref.at[block], recv_sem.at[block])


def reduce_scatter(n_seq, rows_ref, w_ref, fetch, own_ref, y_send, y_recv, z_send, z_recv, sems,
                   finish, lag):
    ys_sem, yr_sem, zs_sem, zr_sem = sems
    pieces, _, width = w_ref.shape
    seq = lax.axis_index("seq")
    high_count = n_seq // LOW
    high, low = seq // LOW, lax.rem(seq, LOW)
    half = rows_ref.shape[0] // LOW
    row_share = half // high_count
    wire = y_send.dtype

    def y_copy(p):
        return pltpu.make_async_remote_copy(
            src_ref=y_send.at[p], dst_ref=y_recv.at[p], send_sem=ys_sem.at[p],
            recv_sem=yr_sem.at[p], device_id={"seq": seq + 1 - 2 * low}, device_id_type=MESH)

    def z_copy(p, i):
        peer = lax.rem(high + i, high_count)
        return pltpu.make_async_remote_copy(
            src_ref=z_send.at[p, peer], dst_ref=z_recv.at[p, i - 1], send_sem=zs_sem.at[p, i - 1],
            recv_sem=zr_sem.at[p, i - 1], device_id={"seq": peer * LOW + low},
            device_id_type=MESH)

    def multiply(p, carry):
        fetch(p).wait()
        theirs = rows_ref[pl.ds(pl.multiple_of((1 - low) * half, half), half), :]
        y_send[p] = jnp.dot(theirs, w_ref[p], preferred_element_type=jnp.float32).astype(wire)
        y_copy(p).start()
        mine = rows_ref[pl.ds(pl.multiple_of(low * half, half), half), :]
        own_ref[p] = jnp.dot(mine, w_ref[p], preferred_element_type=jnp.float32).reshape(
            high_count, row_share, width
        )
        return carry

    def spread(p):
        y_copy(p).wait_recv()
        summed = own_ref[p] + y_recv[p].astype(jnp.float32).reshape(high_count, row_share, width)
        own_ref[p] = summed
        z_send[p] = summed.astype(wire)
        for i in range(1, high_count):
            z_copy(p, i).start()

    def collect(p):
        total = own_ref[p, high]
        for i in range(1, high_count):
            z_copy(p, i).wait_recv()
            total = total + z_recv[p, i - 1].astype(jnp.float32)
        finish(p, total)

    def first(p, carry):
        spread(p)
        return carry

    def step(p, carry):
        spread(p)
        collect(p - lag)
        return carry

    def last(p, carry):
        collect(p)
        return carry

    def drain(p, carry):
        y_copy(p).wait_send()
        for i in range(1, high_count):
            z_copy(p, i).wait_send()
        return carry

    lax.fori_loop(0, pieces, multiply, 0)
    lag = min(lag, pieces)
    lax.fori_loop(0, lag, first, 0)
    lax.fori_loop(lag, pieces, step, 0)
    lax.fori_loop(pieces - lag, pieces, last, 0)
    return lambda: lax.fori_loop(0, pieces, drain, 0)


def step_kernel(n_seq, n_grp, hidden_ref, group_of_ref, len_ref, table_ref, bias_ref,
                place_ref, w_in_hbm, w_out_hbm, k_hbm, v_hbm, mixed_ref,
                perm_ref, back_ref, cos_ref, sin_ref, slot_ref, slots_ref,
                key_ref, value_ref, w_in_ref, w_out_ref, hid_all, rows_ref, p_own, p_ys, p_yr,
                p_zs, p_zr, turned_ref, d_send, d_recv, x_ref, wide_ref, block_ref, q_ref, nv_send,
                nv_ref, page_ref, stat_ref, o_send, o_all, s_all, att_ref, att_all, m_own, m_ys,
                m_yr, m_zs, m_zr, slot_sem, w_in_sem, w_out_sem, kv_sem, hs_sem, hr_sem, p_ys_sem, p_yr_sem,
                p_zs_sem, p_zr_sem, ds_sem, dr_sem, qs_sem, qf_sem, qr_sem, ns_sem, nr_sem, os_sem,
                or_sem, ss_sem, sr_sem, as_sem, ar_sem, m_ys_sem, m_yr_sem, m_zs_sem, m_zr_sem):
    seq, grp = lax.axis_index("seq"), lax.axis_index("grp")
    high_count = n_seq // LOW
    high, low = seq // LOW, lax.rem(seq, LOW)
    pair = seq + 1 - 2 * low
    in_pieces, depth, in_width = w_in_ref.shape
    out_pieces, out_depth, out_width = w_out_ref.shape
    parts = hid_all.shape[0]
    share = block_ref.shape[0]
    piece_heads = in_width // HD
    block_heads = in_pieces * piece_heads
    head_share = HQ // n_seq
    group_q = HQ // KVH
    group_size = share * n_seq

    def in_fetch(p):
        return pltpu.make_async_copy(
            w_in_hbm.at[:, pl.ds(pl.multiple_of(p * in_width, in_width), in_width)],
            w_in_ref.at[p], w_in_sem.at[p])

    def out_fetch(p):
        return pltpu.make_async_copy(
            w_out_hbm.at[:, pl.ds(pl.multiple_of(p * out_width, out_width), out_width)],
            w_out_ref.at[p], w_out_sem.at[p])

    key_copy = pltpu.make_async_copy(k_hbm.at[0], key_ref, kv_sem.at[0])
    value_copy = pltpu.make_async_copy(v_hbm.at[0], value_ref, kv_sem.at[1])
    for p in range(in_pieces):
        in_fetch(p).start()
    greet(n_seq, n_grp)
    order = serve_order(n_seq, n_grp, group_of_ref, perm_ref)
    greeted(n_seq, n_grp)

    sends = []
    part = depth // parts
    for a in range(parts):
        sends += gather_start(n_grp, hidden_ref.at[:, a * part : (a + 1) * part], hid_all.at[a],
                              hs_sem.at[a], hr_sem.at[a])
    key_copy.start()
    value_copy.start()
    for p in range(out_pieces):
        out_fetch(p).start()
    serve_tables(n_seq, n_grp, order, group_of_ref, len_ref, table_ref, place_ref, back_ref,
                 cos_ref, sin_ref, slot_ref)
    slot_copy = pltpu.make_async_copy(slot_ref, slots_ref, slot_sem)
    slot_copy.start()
    for a in range(parts):
        sends += gather_relay(n_grp, hid_all.at[a], hs_sem.at[a], hr_sem.at[a])
    for a in range(parts):
        gather_finish(n_grp, hid_all.at[a], hr_sem.at[a])
        rows_ref[:, a * part : (a + 1) * part] = jnp.dot(
            perm_ref[...], hid_all[a].reshape(-1, part), preferred_element_type=jnp.float32
        ).astype(jnp.bfloat16)

    def turn(p, total):
        for k in range(piece_heads):
            head = p * piece_heads + k
            values = total[:, k * HD : (k + 1) * HD] + bias_ref[pl.ds(head, 1), :]
            rotated = values * cos_ref[...] + pltpu.roll(values, HD // 2, 1) * sin_ref[...]
            values = jnp.where(grp * block_heads + head < HQ + KVH, rotated, values)
            for g in range(n_grp):
                turned_ref[g, pl.ds(head, share, stride=block_heads), :] = values[
                    g * share : (g + 1) * share
                ]

    drain_in = reduce_scatter(n_seq, rows_ref, w_in_ref, in_fetch, p_own, p_ys, p_yr, p_zs, p_zr,
                              (p_ys_sem, p_yr_sem, p_zs_sem, p_zr_sem), turn, 2)

    d_send[...] = turned_ref[...].astype(jnp.bfloat16)
    head_sends = []
    for i in range(1, n_grp):
        peer = lax.rem(grp + i, n_grp)
        head_sends.append(
            send(d_send.at[peer], d_recv.at[i - 1], ds_sem.at[i - 1], dr_sem.at[i - 1], "grp", peer)
        )
    x_ref[grp] = d_send[grp].astype(jnp.float32)
    for i in range(1, n_grp):
        head_sends[i - 1].wait_recv()
        x_ref[lax.rem(grp + n_grp - i, n_grp)] = d_recv[i - 1].astype(jnp.float32)
    sends += head_sends

    def head_rows(head):
        return x_ref[head // block_heads, pl.ds(head % block_heads, share, stride=block_heads), :]

    for head in range(HQ):
        wide_ref[pl.ds(head, share, stride=HQ), :] = head_rows(head)
    block_ref[...] = wide_ref[...].reshape(share, HQ, HD).astype(jnp.bfloat16)

    chunks = qr_sem.shape[1]
    chunk = share // chunks

    def rows_of(index, c):
        return q_ref.at[pl.ds(index * share + c * chunk, chunk)]

    for c in range(chunks):
        source = block_ref.at[pl.ds(c * chunk, chunk)]
        for i in range(1, high_count):
            peer = lax.rem(high + i, high_count) * LOW + low
            sends.append(send(source, rows_of(seq, c), qs_sem.at[i - 1, c], qr_sem.at[seq, c],
                              "seq", peer))
        sends.append(send(source, rows_of(seq, c), qs_sem.at[high_count - 1, c], qr_sem.at[seq, c],
                          "seq", pair))
    q_ref[pl.ds(seq * share, share)] = block_ref[...]
    for c in range(chunks):
        for i in range(1, high_count):
            block = lax.rem(high + high_count - i, high_count) * LOW + low
            arrived(rows_of(block, c), qr_sem.at[block, c])
            sends.append(send(rows_of(block, c), rows_of(block, c), qf_sem.at[i - 1, c],
                              qr_sem.at[block, c], "seq", pair))

    lane = lax.broadcasted_iota(jnp.int32, (share, HD), 1)
    for peer in range(n_seq):
        kv = peer * head_share // group_q
        scores = jnp.zeros((share, HD), jnp.float32)
        for k in range(head_share):
            head = peer * head_share + k
            key = head_rows(HQ + head // group_q)
            score = jnp.sum(head_rows(head) * key, axis=1, keepdims=True) * (HD**-0.5)
            scores = jnp.where(lane == k, score, scores)
        nv_send[peer, 0] = scores
        nv_send[peer, 1] = head_rows(HQ + KVH + kv)
    for i in range(1, n_seq):
        peer = lax.rem(seq + i, n_seq)
        sends.append(
            send(nv_send.at[peer], nv_ref.at[seq], ns_sem.at[i - 1], nr_sem.at[seq], "seq", peer)
        )
    nv_ref[seq] = nv_send[seq]
    stat_ref[...] = jnp.zeros_like(stat_ref)
    slot_copy.wait()
    key_copy.wait()
    value_copy.wait()
    for h in range(high_count):
        for c in range(chunks):
            block = h * LOW + 1 - low
            arrived(rows_of(block, c), qr_sem.at[block, c])

    blocks, block_rows, _ = o_send.shape
    block_pages = block_rows // HQ
    pool_pages = blocks * block_pages
    unroll = math.gcd(block_pages, 8)
    place = lax.broadcasted_iota(jnp.int32, (HQ, PAGE), 1)
    spot = lax.broadcasted_iota(jnp.int32, (HQ, HD), 1)
    own_rows = head_share * block_pages

    def attend(first, step, carry):
        stat = stat_ref[...].reshape(HQ, HD)
        for j in range(unroll):
            within = step * unroll + j
            page = first + within
            page_live, owner = slots_ref[page, 0] // group_size, slots_ref[page, 0] % group_size
            alive = place < page_live
            query = q_ref[owner]
            start = pl.multiple_of(page * PAGE, PAGE)
            keys = key_ref[pl.ds(start, PAGE), :]
            values = value_ref[pl.ds(start, PAGE), :]
            scores = jnp.concatenate(
                [
                    lax.dot_general(
                        query[h * group_q : (h + 1) * group_q],
                        keys[:, h * HD : (h + 1) * HD],
                        (((1,), (1,)), ((), ())),
                        preferred_element_type=jnp.float32,
                    )
                    for h in range(KVH)
                ],
                axis=0,
            ) * (HD**-0.5)
            scores = jnp.where(alive, scores, neg_fill)
            page_max = jnp.max(scores, axis=1, keepdims=True)
            weights = jnp.where(alive, jnp.exp(scores - page_max), 0.0)
            page_total = jnp.sum(weights, axis=1, keepdims=True)
            rounded = weights.astype(jnp.bfloat16)
            page_out = jnp.concatenate(
                [
                    jnp.dot(
                        rounded[h * group_q : (h + 1) * group_q],
                        values[:, h * HD : (h + 1) * HD],
                        preferred_element_type=jnp.float32,
                    )
                    for h in range(KVH)
                ],
                axis=0,
            )
            page_ref[pl.ds(within, HQ, stride=block_pages), :] = page_out
            holder = jnp.where(page_live > 0, owner, -1).astype(jnp.float32)
            stat = jnp.where(spot == page, page_max, stat)
            stat = jnp.where(spot == pool_pages + page, page_total, stat)
            stat = jnp.where(spot == 2 * pool_pages + page, holder, stat)
        stat_ref[...] = stat.reshape(stat_ref.shape)
        return carry

    for b in range(blocks):
        lax.fori_loop(
            0, block_pages // unroll, functools.partial(attend, b * block_pages), 0
        )
        o_send[b] = page_ref[...].astype(jnp.bfloat16)
        for i in range(1, n_seq):
            peer = lax.rem(seq + i, n_seq)
            if b == blocks - 1:
                sends.append(send(stat_ref.at[peer], s_all.at[seq], ss_sem.at[i - 1],
                                  sr_sem.at[seq], "seq", peer))
            sends.append(send(o_send.at[b, pl.ds(peer * own_rows, own_rows)], o_all.at[seq, b],
                              os_sem.at[i - 1, b], or_sem.at[seq, b], "seq", peer))
        o_all[seq, b] = o_send[b, pl.ds(pl.multiple_of(seq * own_rows, own_rows), own_rows)]
    s_all[seq] = stat_ref[seq]

    for i in range(1, n_seq):
        block = lax.rem(seq + i, n_seq)
        arrived(nv_ref.at[block], nr_sem.at[block])
        arrived(s_all.at[block], sr_sem.at[block])
    packed = HD // pool_pages
    slots = n_seq * pool_pages
    spot = lax.broadcasted_iota(jnp.int32, (head_share, HD), 1) // pool_pages

    def lined_up(field):
        tiles = []
        for first in range(0, n_seq, packed):
            tile = jnp.zeros((head_share, HD), jnp.float32)
            for k in range(packed):
                shift = (HD + (k - field) * pool_pages) % HD
                source = s_all[first + k]
                tile = jnp.where(spot == k, pltpu.roll(source, shift, 1) if shift else source, tile)
            tiles.append(tile)
        return jnp.concatenate(tiles, axis=1)

    tops, totals, holders = lined_up(0), lined_up(1), lined_up(2)
    request = lax.broadcasted_iota(jnp.int32, (group_size, slots), 0).astype(jnp.float32)
    held = request == holders[:1, :]
    fresh_scores = nv_ref[:, 0].reshape(group_size, HD)
    fresh_values = nv_ref[:, 1].reshape(group_size, HD)
    for b in range(blocks):
        for i in range(1, n_seq):
            block = lax.rem(seq + i, n_seq)
            arrived(o_all.at[block, b], or_sem.at[block, b])
    parts = att_all.shape[0]
    part_heads = head_share // parts
    part = part_heads * HD
    for a in range(parts):
        for m in range(part_heads):
            k = a * part_heads + m
            top = jnp.where(held, tops[k : k + 1, :], neg_fill)
            fresh = fresh_scores[:, k : k + 1]
            peak = jnp.maximum(jnp.max(top, axis=1, keepdims=True), fresh)
            factor = jnp.where(held, jnp.exp(top - peak), 0.0)
            fresh_weight = jnp.exp(fresh - peak)
            denominator = (
                jnp.sum(factor * totals[k : k + 1, :], axis=1, keepdims=True) + fresh_weight
            )
            coarse = factor.astype(jnp.bfloat16)
            fine = (factor - coarse.astype(jnp.float32)).astype(jnp.bfloat16)
            outs = o_all[:, :, k * block_pages : (k + 1) * block_pages, :].reshape(slots, HD)
            numerator = (
                jnp.dot(coarse, outs, preferred_element_type=jnp.float32)
                + jnp.dot(fine, outs, preferred_element_type=jnp.float32)
                + fresh_weight * fresh_values
            )
            att_ref[a, :, m * HD : (m + 1) * HD] = (numerator / denominator).astype(jnp.bfloat16)
        sends += gather_start(n_grp, att_ref.at[a], att_all.at[a], as_sem.at[a], ar_sem.at[a])
    for a in range(parts):
        sends += gather_relay(n_grp, att_all.at[a], as_sem.at[a], ar_sem.at[a])
    for a in range(parts):
        gather_finish(n_grp, att_all.at[a], ar_sem.at[a])
        rows_ref[:, a * part : (a + 1) * part] = jnp.dot(
            back_ref[...], att_all[a].reshape(-1, part), preferred_element_type=jnp.float32
        ).astype(jnp.bfloat16)

    def keep(p, total):
        mixed_ref[:, pl.ds(pl.multiple_of(p * out_width, out_width), out_width)] = total.astype(
            jnp.bfloat16
        )

    drain_out = reduce_scatter(n_seq, rows_ref.at[:, :out_depth], w_out_ref, out_fetch, m_own,
                               m_ys, m_yr, m_zs, m_zr, (m_ys_sem, m_yr_sem, m_zs_sem, m_zr_sem),
                               keep, 8)
    drain_in()
    drain_out()
    for copy in sends:
        copy.wait_send()


def run_step(n_seq, n_grp, hidden, group_of, lengths, table, bias, places, w_qkv, w_out,
             k_cache, v_cache):
    group_size, depth = hidden.shape
    request_total = table.shape[0]
    in_cols = w_qkv.shape[1]
    out_depth, out_cols = w_out.shape
    in_pieces, out_pieces = math.gcd(in_cols // HD, 10), math.gcd(out_cols // HD, 8)
    in_width, out_width = in_cols // in_pieces, out_cols // out_pieces
    half = request_total // LOW
    high_count = n_seq // LOW
    row_share = half // high_count
    share = row_share // n_grp
    head_share = HQ // n_seq
    block_rows = share * in_cols // HD
    positions = k_cache.shape[1]
    pool_pages = positions // PAGE
    block_pages = math.gcd(pool_pages, 8)
    blocks = pool_pages // block_pages
    chunks = math.gcd(share, 4)
    parts = 2
    bf16, f32 = jnp.bfloat16, jnp.float32
    dma = pltpu.SemaphoreType.DMA
    vmem = pl.BlockSpec(memory_space=pltpu.VMEM)
    hbm = pl.BlockSpec(memory_space=pl.ANY)
    scratch = [
        ((request_total, request_total), bf16),
        ((request_total, request_total), bf16),
        ((row_share, HD), f32),
        ((row_share, HD), f32),
        ((pool_pages, HD), jnp.int32),
    ]
    smem_scratch = [pltpu.SMEM((pool_pages, HD), jnp.int32)]
    more_scratch = [
        ((positions, KVH * HD), bf16),
        ((positions, KVH * HD), bf16),
        ((in_pieces, depth, in_width), bf16),
        ((out_pieces, out_depth, out_width), bf16),
        ((parts, n_grp, group_size, depth // parts), bf16),
        ((request_total, max(depth, out_depth)), bf16),
        ((in_pieces, high_count, row_share, in_width), f32),
        ((in_pieces, half, in_width), f32),
        ((in_pieces, half, in_width), f32),
        ((in_pieces, high_count, row_share, in_width), f32),
        ((in_pieces, high_count - 1, row_share, in_width), f32),
        ((n_grp, block_rows, HD), f32),
        ((n_grp, block_rows, HD), bf16),
        ((n_grp - 1, block_rows, HD), bf16),
        ((n_grp, block_rows, HD), f32),
        ((share * HQ, HD), f32),
        ((share, HQ, HD), bf16),
        ((group_size, HQ, HD), bf16),
        ((n_seq, 2, share, HD), f32),
        ((n_seq, 2, share, HD), f32),
        ((HQ * block_pages, HD), f32),
        ((n_seq, head_share, HD), f32),
        ((blocks, HQ * block_pages, HD), bf16),
        ((n_seq, blocks, head_share * block_pages, HD), bf16),
        ((n_seq, head_share, HD), f32),
        ((parts, group_size, out_depth // parts), bf16),
        ((parts, n_grp, group_size, out_depth // parts), bf16),
        ((out_pieces, high_count, row_share, out_width), f32),
        ((out_pieces, half, out_width), bf16),
        ((out_pieces, half, out_width), bf16),
        ((out_pieces, high_count, row_share, out_width), bf16),
        ((out_pieces, high_count - 1, row_share, out_width), bf16),
    ]
    sems = [
        (in_pieces,), (out_pieces,), (2,), (parts, 2 * n_grp), (parts, n_grp),
        (in_pieces,), (in_pieces,), (in_pieces, high_count - 1), (in_pieces, high_count - 1),
        (n_grp - 1,), (n_grp - 1,), (high_count, chunks), (high_count - 1, chunks),
        (n_seq, chunks), (n_seq - 1,), (n_seq,), (n_seq - 1, blocks), (n_seq, blocks),
        (n_seq - 1,), (n_seq,), (parts, 2 * n_grp), (parts, n_grp),
        (out_pieces,), (out_pieces,), (out_pieces, high_count - 1), (out_pieces, high_count - 1),
    ]
    return pl.pallas_call(
        functools.partial(step_kernel, n_seq, n_grp),
        out_shape=jax.ShapeDtypeStruct((row_share, out_cols), bf16),
        in_specs=[vmem] * 6 + [hbm] * 4,
        out_specs=vmem,
        scratch_shapes=[pltpu.VMEM(s, t) for s, t in scratch]
        + smem_scratch
        + [pltpu.VMEM(s, t) for s, t in more_scratch]
        + [dma(())]
        + [dma(s) for s in sems],
        compiler_params=pltpu.CompilerParams(
            collective_id=0, has_side_effects=True, vmem_limit_bytes=60 * 1024 * 1024
        ),
        cost_estimate=pl.CostEstimate(
            flops=2 * request_total * depth * in_cols,
            bytes_accessed=2 * depth * in_cols,
            transcendentals=0,
        ),
    )(hidden, group_of, lengths, table, bias, places, w_qkv, w_out, k_cache, v_cache)


def shards(hidden, w_qkv, b_qkv, w_out, k_cache, v_cache, lengths, page_table, positions, group_of):
    n_seq, n_grp = lax.axis_size("seq"), lax.axis_size("grp")
    return run_step(
        n_seq, n_grp, hidden, group_of[None, :], lengths[None, :], page_table,
        b_qkv.reshape(-1, HD), positions, w_qkv, w_out, k_cache, v_cache
    )


def solution(mesh):
    placed = (
        P("grp", "seq"),
        P("seq", "grp"),
        P("grp"),
        P("seq", "grp"),
        P("grp", "seq", None),
        P("grp", "seq", None),
        P(),
        P(),
        P(),
        P(),
    )
    return jax.shard_map(
        shards, mesh=mesh, in_specs=placed, out_specs=P("seq", "grp"), check_vma=False
    )
```
